512 devices in a mesh: gx: 16 (over y, core), gy: 4 (over x), gz: 8 (over z).
Axes of the slice: x: 4, y: 8, z: 8, core: 2. Of those that a mesh axis runs over, the one named last changes fastest.
Arguments:
- face_blocks: float32 [16, 4, 8, 24, 16384], P('gx', 'gy', 'gz'), may hold values from -6 to 6
- owner_rank: int32 [16, 4, 8, 24, 1], P('gx', 'gy', 'gz'), may hold values from 0 to 15; in each aligned block of 24 rows (0 to 23, 24 to 47, ..., all dimensions but the last counted through in order) at most 2 rows name the same one
- owner_tile: int32 [16, 4, 8, 24], P('gx', 'gy', 'gz'), may hold values from 0 to 31
- live_count: int32 [16, 4, 8], P('gx', 'gy', 'gz'), may hold values from 1 to 24, as said below
- right_side: float32 [256, 256, 1024], P('gx', 'gy', 'gz'), may hold values from -8 to 8
- diagonal: float32 [256, 256, 1024], P('gx', 'gy', 'gz'), may hold values from 0.05 to 1
Outputs:
- solution_field: float32 [256, 256, 1024], P('gx', 'gy', 'gz')
- residual: float32 [256, 256, 1024], P('gx', 'gy', 'gz')
The draws below stay inside these ranges and needn't reach their ends.
Inputs may be any that keep to these rules, and one draw needn't show every extreme that they name: `owner_rank`: on one device no owner is named by more than 2 of the 24 slots, live or not; some owner is named exactly 2 times on some devices. `live_count`: some device has all 24 slots live in every draw.
All inputs are finite; a program needn't handle non-finite values.
Results may differ from the reference program's by a relative error of at most 0.00012.
Values sent between devices are 32-bit elements; how exact they have to be, the bound alone decides.
A program may use at most 64 MiB of HBM per device.

```python
import math
import jax
import jax.numpy as jnp
import numpy as np

BLK = 128
CAP = 2
ITERS = 2
CX = 16
NB = 24
NX = 256
NY = 256
NZ = 1024
N_GX = 16
N_GY = 4
N_GZ = 8


def draw_live_count(key, part):
    counts = jax.random.randint(key, (N_GX, N_GY, N_GZ), 1, NB + 1)
    return counts.at[0, 0, 0].set(NB).astype(jnp.int32)


def set_ends(array, key, smallest, largest):
    place = [jax.random.randint(jax.random.fold_in(key, axis), (), 0, length) for axis, length in enumerate(array.shape)]
    main_axis = array.shape.index(max(array.shape))
    neighbour = place[:main_axis] + [(place[main_axis] + 1) % array.shape[main_axis]] + place[main_axis + 1:]
    return array.at[tuple(place)].set(smallest).at[tuple(neighbour)].set(largest)


def block_scale(rng, dims, split, low, top_value):
    gain = 1.0
    for axis_at, parts in split:
        heights = jax.random.uniform(jax.random.fold_in(jax.random.fold_in(rng, 6), axis_at), (parts,), jnp.float32, low / len(split), top_value / len(split))
        gain = gain * jnp.repeat(jnp.exp(heights), dims[axis_at] // parts).reshape((-1,) + (1,) * (len(dims) - 1 - axis_at))
    return gain


def deal_out(key, own, number, rows, count, top, bound, skew):
    sequence = jax.random.permutation(key, count)
    packed, ordinary = portions_of(count, rows * top, bound, skew, True), portions_of(count, rows * top, bound, skew, False)
    places = jnp.arange(count)

    def named(lengths, turn):
        used = int((lengths > 0).sum())
        fixed = max(1, used // 4)
        shifted = fixed + (places - fixed + turn * (used - fixed)) % max(1, count - fixed)
        return jnp.zeros((count,), jnp.int32).at[sequence[jnp.where(places < fixed, places, shifted)]].set(jnp.asarray(lengths, jnp.int32))

    lengths = jnp.where(number % 4 == 0, named(packed, number // 4), named(ordinary, number - number // 4 - 1))
    mixed = jax.random.permutation(jax.random.fold_in(own, 3), count)
    donor, sink = mixed[0:count // 2 * 2:2], mixed[1:count // 2 * 2:2]
    margin = jnp.minimum(lengths[donor] - 1, bound - lengths[sink]) // 2
    margin = jnp.where((donor == sequence[0]) | (sink == sequence[0]) | (lengths[sink] == 0), 0, jnp.maximum(margin, 0))
    shifted = jax.random.randint(jax.random.fold_in(own, 4), (count // 2,), 0, 1 << 20) % (margin + 1)
    lengths = lengths.at[donor].add(-shifted).at[sink].add(shifted)
    members = jnp.searchsorted(jnp.cumsum(lengths), jnp.arange(rows * top), side="right").astype(jnp.int32)
    listing = members.reshape(top, rows).T
    listing = listing[jax.random.permutation(jax.random.fold_in(own, 1), rows)]
    turn = jax.random.randint(jax.random.fold_in(own, 2), (rows, 1), 0, top)
    return jnp.take_along_axis(listing, (jnp.arange(top)[None, :] + turn) % top, axis=1)


def portions_of(number_of, total, limit, slope, full):
    portions = [(1 << 20) // math.isqrt(standing ** slope) + 1 for standing in range(1, number_of + 1)]
    largest = limit if full else min(limit, max(-(-total // number_of), total * portions[0] // sum(portions)))
    least = 1 if total - largest >= number_of - 1 else 0
    given, spare = [largest] + [least] * (number_of - 1), total - largest - least * (number_of - 1)
    while spare > 0:
        movable = [i for i in range(1, number_of) if given[i] < largest] or [i for i in range(1, number_of) if given[i] < limit]
        mass, left = sum([portions[i] for i in movable]), spare
        for i in movable:
            more = min(limit - given[i], max(1, left * portions[i] // mass), spare)
            given[i] = given[i] + more
            spare = spare - more
    return np.array(given)


def scatter_about(own_key, dims, deviation, reach, split=(), held_as=jnp.bfloat16):
    values = jax.random.normal(own_key, dims, jnp.float32) * deviation
    if len(split) > 0:
        values = block_scale(own_key, dims, split, -0.22, 0.18) * values
    return jnp.clip(values, min=-reach, max=reach).astype(held_as)


def setup_inputs(seed: int = 0) -> dict:
    keys = jax.random.split(jax.random.key(seed), 7)
    face_blocks = scatter_about(keys[0], (N_GX, N_GY, N_GZ, NB, BLK * BLK), 1.0, 6.0, ((0, 16), (1, 4), (2, 8)), jnp.float32)
    owner_rank_keys = jax.random.split(jax.random.fold_in(keys[1], 1), N_GX * N_GY * N_GZ * NB // NB)
    owner_rank_turns = jax.random.permutation(jax.random.fold_in(keys[1], 3), N_GX * N_GY * N_GZ * NB // NB)
    owner_rank = jax.vmap(lambda own, number: deal_out(jax.random.fold_in(keys[1], 2), own, number, NB, N_GX, 1, CAP, 2))(owner_rank_keys, owner_rank_turns).reshape((N_GX, N_GY, N_GZ, NB, 1))
    owner_tile = set_ends(jax.random.randint(keys[2], (N_GX, N_GY, N_GZ, NB), 0, 2 * CX), jax.random.fold_in(keys[2], 1), 0, (2 * CX) - 1).astype(jnp.int32)
    live_count = draw_live_count(jax.random.fold_in(keys[6], 71), 0)
    right_side = scatter_about(keys[4], (NX, NY, NZ), 1.0, 8.0, ((0, 16), (1, 4), (2, 8)), jnp.float32)
    diagonal = jnp.clip(jnp.exp(math.log(1.0) - 2.9957323 * jax.random.uniform(keys[5], (NX, NY, NZ), jnp.float32) ** block_scale(keys[5], (NX, NY, NZ), ((0, 16), (1, 4), (2, 8)), -0.2, 0.2)), 0.05, 1.0)
    return dict(face_blocks=face_blocks, owner_rank=owner_rank, owner_tile=owner_tile, live_count=live_count, right_side=right_side, diagonal=diagonal)


def restrict(values):
    half = BLK // 2
    shaped = values.reshape(values.shape[:-1] + (half, 2, half, 2))
    summed = 0.25 * jnp.sum(shaped, axis=(-3, -1))
    return summed.reshape(values.shape[:-1] + (half * half,))


def operate(field, diagonal):
    padded = jnp.pad(field, 1)
    beside = padded[2:, 1:-1, 1:-1] + padded[:-2, 1:-1, 1:-1]
    beside = beside + padded[1:-1, 2:, 1:-1] + padded[1:-1, :-2, 1:-1]
    beside = beside + padded[1:-1, 1:-1, 2:] + padded[1:-1, 1:-1, :-2]
    return (6.0 + diagonal) * field - beside


def reference(face_blocks, owner_rank, owner_tile, live_count, right_side, diagonal):
    half = BLK // 2
    restricted = restrict(face_blocks)
    slots = jnp.arange(NB, dtype=jnp.int32)
    living = (slots[None, None, None, :] < live_count[..., None]).astype(jnp.float32)
    restricted = restricted * living[..., None]
    row_y = jnp.broadcast_to(jnp.arange(N_GY, dtype=jnp.int32)[None, :, None, None], (N_GX, N_GY, N_GZ, NB))
    row_z = jnp.broadcast_to(jnp.arange(N_GZ, dtype=jnp.int32)[None, None, :, None], (N_GX, N_GY, N_GZ, NB))
    target = owner_rank[..., 0].astype(jnp.int32)
    gathered = jnp.zeros((N_GX, N_GY, N_GZ, 2 * CX, half * half), jnp.float32)
    gathered = gathered.at[target, row_y, row_z, owner_tile.astype(jnp.int32)].add(restricted)
    shaped = gathered.reshape(N_GX, N_GY, N_GZ, CX, 2, half, half)
    source = jnp.transpose(shaped, (0, 3, 1, 5, 2, 4, 6)).reshape(NX, NY, NZ)
    load = right_side + source
    solution_field = jnp.zeros_like(load)
    residual, direction = load, load
    norm_now = jnp.sum(residual * residual)
    for iteration in range(ITERS):
        image = operate(direction, diagonal)
        alpha = norm_now / jnp.sum(direction * image)
        solution_field = solution_field + alpha * direction
        residual = residual - alpha * image
        norm_next = jnp.sum(residual * residual)
        direction = residual + (norm_next / norm_now) * direction
        norm_now = norm_next
    return solution_field, residual
```

```python
import functools

import jax
import jax.numpy as jnp
from jax import lax
from jax.experimental import pallas as pl
from jax.experimental.pallas import tpu as pltpu
from jax.sharding import PartitionSpec as P

NB = 24
BLK = 128
HALF = BLK // 2
CX = 16
F32 = jnp.float32
MESH = pl.DeviceIdType.MESH
TOP = 8


def body(
    n_gx, n_gy, n_gz,
    count_hbm, rank_hbm, tile_hbm, face_ref, rhs_ref, diag_ref,
    x_out, r_out,
    count_ref, rank_ref, tile_ref, live_rank, face, rows, pair, sbuf, rbuf, stag, rtag,
    v0, v1, v2, diag, ysend, yrecv, zsend, zrecv,
    part_a, part_b, recv_a, recv_b,
    in_sem, s_sem, r_sem, st_sem, rt_sem, hs_sem, hr_sem,
    as_sem, ar_sem, bs_sem, br_sem,
):
    gx, gy, gz = lax.axis_index("gx"), lax.axis_index("gy"), lax.axis_index("gz")
    chips = n_gx // 2
    chip, core = gx // 2, gx % 2
    plane_n = n_gy * n_gz
    plane_me = gy * n_gz + gz
    barrier = pltpu.get_barrier_semaphore()

    small_copies = [
        pltpu.make_async_copy(src, dst, in_sem.at[6 + i])
        for i, (src, dst) in enumerate(
            ((count_hbm, count_ref), (rank_hbm, rank_ref), (tile_hbm, tile_ref))
        )
    ]
    for c in small_copies:
        c.start()
    pieces = 4
    width = face.shape[1] // pieces
    face_copies = [
        pltpu.make_async_copy(
            face_ref.at[:, pl.ds(i * width, width)], face.at[:, pl.ds(i * width, width)], in_sem.at[i]
        )
        for i in range(pieces)
    ]
    for c in face_copies:
        c.start()
    rhs_copy = pltpu.make_async_copy(
        rhs_ref, v0.at[pl.ds(1, CX), pl.ds(TOP, HALF), :], in_sem.at[pieces]
    )
    rhs_copy.start()
    diag_copy = pltpu.make_async_copy(diag_ref, diag, in_sem.at[pieces + 1])
    diag_copy.start()

    zrecv[...] = jnp.zeros_like(zrecv)
    yrecv[...] = jnp.zeros_like(yrecv)

    @pl.loop(1, n_gx)
    def _(k):
        pl.semaphore_signal(
            barrier, inc=1, device_id=(lax.rem(gx + k, n_gx), gy, gz), device_id_type=MESH
        )

    def plane_peer(k):
        q = lax.rem(plane_me + k, plane_n)
        return q // n_gz, lax.rem(q, n_gz)

    @pl.loop(1, plane_n)
    def _(k):
        py, pz = plane_peer(k)
        pl.semaphore_signal(barrier, inc=1, device_id=(gx, py, pz), device_id_type=MESH)

    lane = lax.broadcasted_iota(jnp.int32, (8, BLK), 1)
    k_at = lax.broadcasted_iota(jnp.int32, (2 * BLK, BLK), 0)
    c_at = lax.broadcasted_iota(jnp.int32, (2 * BLK, BLK), 1)
    hit = (k_at // BLK == c_at // HALF) & ((k_at % BLK) // 2 == c_at % HALF)
    pair[...] = jnp.where(hit, 0.25, 0.0).astype(jnp.bfloat16)
    rows[NB] = jnp.zeros((HALF, BLK), F32)
    by_row = rows.reshape((NB + 1) * HALF, BLK)
    for c in small_copies:
        c.wait()
    count = count_ref[0]
    for s in range(NB):
        live_rank[s] = jnp.where(s < count, rank_ref[s], -1)

    pl.semaphore_wait(barrier, n_gx - 1 + plane_n - 1)

    @pl.when(gx == 0)
    def _():
        for v in (v0, v1):
            v[0, pl.ds(TOP, HALF), :] = jnp.zeros((HALF, BLK), F32)

    @pl.when(gx == n_gx - 1)
    def _():
        for v in (v0, v1):
            v[CX + 1, pl.ds(TOP, HALF), :] = jnp.zeros((HALF, BLK), F32)

    per = HALF // pieces
    for i in range(pieces):
        face_copies[i].wait()

        @pl.loop(0, per // 4)
        def _(r4):
            for u in range(4):
                r = i * per + r4 * 4 + u
                at = pl.multiple_of(r * 2 * BLK, 2 * BLK)
                both = face[:, pl.ds(at, BLK)] + face[:, pl.ds(at + BLK, BLK)]
                for g in range(NB // 8):
                    by_row[pl.ds(g * 8 * HALF + r, 8, stride=HALF), :] = both[g * 8 : g * 8 + 8]

    def step_chip(t):
        j = t // 2
        return (1 - 2 * (j % 2)) * (chips // 2 - (j + 1) // 2)

    def target_of(t):
        return lax.rem(chip + step_chip(t) + chips, chips) * 2 + lax.rem(core + 1 + t, 2)

    def source_of(t):
        return lax.rem(chip - step_chip(t) + chips, chips) * 2 + lax.rem(core + 1 + t, 2)

    def packed(tgt):
        i0, i1 = jnp.int32(NB), jnp.int32(NB)
        l0, l1 = jnp.int32(0), jnp.int32(0)
        for s in range(NB):
            named = live_rank[s] == tgt
            label = tile_ref[s] + 1
            free = i0 == NB
            first = named & free
            second = named & jnp.logical_not(free)
            i1 = jnp.where(second, s, i1)
            l1 = jnp.where(second, label, l1)
            i0 = jnp.where(first, s, i0)
            l0 = jnp.where(first, label, l0)
        a = rows[i0]
        b = rows[i1]
        w = jnp.concatenate([a, b], axis=1)
        hi = w.astype(jnp.bfloat16)
        rest = w - hi.astype(F32)
        mid = rest.astype(jnp.bfloat16)
        low = (rest - mid.astype(F32)).astype(jnp.bfloat16)
        s = pair[...]
        o = jnp.dot(hi, s, preferred_element_type=F32)
        o = o + jnp.dot(mid, s, preferred_element_type=F32)
        o = o + jnp.dot(low, s, preferred_element_type=F32)
        tag = jnp.where(lane[0:1] < HALF, l0, l1).astype(F32)
        return o, tag

    def tile_copy(t, tgt, slot):
        return pltpu.make_async_remote_copy(
            src_ref=sbuf.at[t], dst_ref=rbuf.at[slot], send_sem=s_sem.at[t], recv_sem=r_sem.at[slot],
            device_id=(tgt, gy, gz), device_id_type=MESH,
        )

    def tag_copy(t, tgt, slot):
        return pltpu.make_async_remote_copy(
            src_ref=stag.at[t], dst_ref=rtag.at[slot], send_sem=st_sem.at[t], recv_sem=rt_sem.at[slot],
            device_id=(tgt, gy, gz), device_id_type=MESH,
        )

    @pl.loop(0, n_gx - 1)
    def _(t):
        tgt = target_of(t)
        o, tag = packed(tgt)
        stag[t] = tag
        sbuf[t] = o
        tag_copy(t, tgt, gx).start()
        tile_copy(t, tgt, gx).start()

    def add_tiles(tile, tag):
        swapped = pltpu.roll(tile, HALF, 1)
        tag = jnp.broadcast_to(tag, (8, BLK))
        tag_swapped = pltpu.roll(tag, HALF, 1)[0:1]
        tag = tag[0:1]
        want = (lane[0:1] // HALF + 1).astype(F32)

        @pl.loop(0, CX // 4)
        def _(x4):
            for u in range(4):
                x = x4 * 4 + u
                here = want + (2 * x).astype(F32)
                m = jnp.broadcast_to(tag == here, (HALF, BLK))
                ms = jnp.broadcast_to(tag_swapped == here, (HALF, BLK))
                more = jnp.where(m, tile, 0.0) + jnp.where(ms, swapped, 0.0)
                v0[1 + x, pl.ds(TOP, HALF), :] = v0[1 + x, pl.ds(TOP, HALF), :] + more

    rhs_copy.wait()
    own, own_tag = packed(gx)
    add_tiles(own, own_tag)

    @pl.loop(0, n_gx - 1)
    def _(t):
        src = source_of(t)
        tag_copy(t, src, src).wait_recv()
        tile_copy(t, src, src).wait_recv()
        add_tiles(rbuf[src], rtag[src])

    diag_copy.wait()

    ends = (lane == 0) | (lane == BLK - 1)
    even = lane % 2 == 0
    inner = pl.ds(TOP, HALF)

    def halo(v, at):
        def x_down():
            return pltpu.make_async_remote_copy(
                src_ref=v.at[1, inner, :], dst_ref=v.at[CX + 1, inner, :],
                send_sem=hs_sem.at[at, 0], recv_sem=hr_sem.at[at, 0],
                device_id=(gx - 1, gy, gz), device_id_type=MESH,
            )

        def x_up():
            return pltpu.make_async_remote_copy(
                src_ref=v.at[CX, inner, :], dst_ref=v.at[0, inner, :],
                send_sem=hs_sem.at[at, 1], recv_sem=hr_sem.at[at, 1],
                device_id=(gx + 1, gy, gz), device_id_type=MESH,
            )

        def y_down():
            return pltpu.make_async_remote_copy(
                src_ref=ysend.at[at, 0], dst_ref=yrecv.at[at, 0],
                send_sem=hs_sem.at[at, 2], recv_sem=hr_sem.at[at, 2],
                device_id=(gx, gy - 1, gz), device_id_type=MESH,
            )

        def y_up():
            return pltpu.make_async_remote_copy(
                src_ref=ysend.at[at, 1], dst_ref=yrecv.at[at, 1],
                send_sem=hs_sem.at[at, 3], recv_sem=hr_sem.at[at, 3],
                device_id=(gx, gy + 1, gz), device_id_type=MESH,
            )

        def z_down():
            return pltpu.make_async_remote_copy(
                src_ref=zsend.at[at, 0], dst_ref=zrecv.at[at, 0],
                send_sem=hs_sem.at[at, 4], recv_sem=hr_sem.at[at, 4],
                device_id=(gx, gy, gz - 1), device_id_type=MESH,
            )

        def z_up():
            return pltpu.make_async_remote_copy(
                src_ref=zsend.at[at, 1], dst_ref=zrecv.at[at, 1],
                send_sem=hs_sem.at[at, 5], recv_sem=hr_sem.at[at, 5],
                device_id=(gx, gy, gz + 1), device_id_type=MESH,
            )

        return (
            (x_down, gx > 0, gx < n_gx - 1),
            (x_up, gx < n_gx - 1, gx > 0),
            (y_down, gy > 0, gy < n_gy - 1),
            (y_up, gy < n_gy - 1, gy > 0),
            (z_down, gz > 0, gz < n_gz - 1),
            (z_up, gz < n_gz - 1, gz > 0),
        )

    def send_faces(v, at):
        faces = halo(v, at)

        def go(which):
            for copy, sends, _ in which:
                @pl.when(sends)
                def _():
                    copy().start()

        go(faces[:2])
        for p in range(CX):
            ysend[at, 0, pl.ds(p, 1), :] = v[1 + p, pl.ds(TOP, 1), :]
            ysend[at, 1, pl.ds(p, 1), :] = v[1 + p, pl.ds(TOP + HALF - 1, 1), :]
        go(faces[2:4])

        def gather(i, carry):
            out = []
            for u in range(2):
                p = 2 * i + u
                acc = None
                for yb in range(HALF // 8):
                    c = jnp.where(ends, v[1 + p, pl.ds(TOP + 8 * yb, 8), :], 0.0)
                    if yb:
                        c = pltpu.roll(c, 16 * yb, 1)
                    acc = c if acc is None else acc + c
                out.append(carry[u] + pltpu.roll(acc, p, 1))
            return tuple(out)

        zero = jnp.zeros((8, BLK), F32)
        v_even, v_odd = lax.fori_loop(0, CX // 2, gather, (zero, zero))
        zsend[at, 0] = jnp.where(even, v_even, v_odd)
        zsend[at, 1] = jnp.where(even, v_odd, v_even)
        go(faces[4:])

    def take_faces(v, at):
        for copy, _, receives in halo(v, at):
            @pl.when(receives)
            def _():
                copy().wait_recv()
        for p in range(CX):
            v[1 + p, pl.ds(TOP + HALF, 1), :] = yrecv[at, 0, pl.ds(p, 1), :]
            v[1 + p, pl.ds(TOP - 1, 1), :] = yrecv[at, 1, pl.ds(p, 1), :]
        right, left = zrecv[at, 0], zrecv[at, 1]
        return jnp.where(even, right, left), jnp.where(even, left, right)

    def apply(v, at, visit, sums):
        sides = take_faces(v, at)

        def planes(i, sums):
            for u in range(2):
                p = 2 * i + u
                side = pltpu.roll(sides[u], lax.rem(BLK - p, BLK), 1)
                for yb in range(HALF // 8):
                    row = TOP + 8 * yb
                    h = pltpu.roll(side, BLK - 16 * yb, 1) if yb else side
                    c = v[1 + p, pl.ds(row, 8), :]
                    near = v[p, pl.ds(row, 8), :] + v[2 + p, pl.ds(row, 8), :]
                    near = near + (v[1 + p, pl.ds(row - 1, 8), :] + v[1 + p, pl.ds(row + 1, 8), :])
                    z_low = pltpu.roll(jnp.where(lane == BLK - 1, h, c), 1, 1)
                    z_high = pltpu.roll(jnp.where(lane == 0, h, c), BLK - 1, 1)
                    near = near + (z_low + z_high)
                    image = (6.0 + diag[p, pl.ds(8 * yb, 8), :]) * c - near
                    sums = visit(p, yb, c, image, sums)
            return sums

        return lax.fori_loop(0, CX // 2, planes, sums)

    zero = jnp.zeros((8, BLK), F32)

    def visit_1(p, yb, c, image, sums):
        v1[1 + p, pl.ds(TOP + 8 * yb, 8), :] = image
        return sums[0] + c * c, sums[1] + c * image, sums[2] + image * image

    def visit_2(p, yb, c, image, sums):
        v2[p, pl.ds(8 * yb, 8), :] = image
        return sums + c * image

    send_faces(v0, 0)
    m0, m1, m2 = apply(v0, 0, visit_1, (zero, zero, zero))
    send_faces(v1, 1)
    m3 = apply(v1, 1, visit_2, zero)

    quarter = lane // 32
    folded = []
    for m in (m0, m1, m2, m3):
        m = m + pltpu.roll(m, 64, 1)
        folded.append(m + pltpu.roll(m, 32, 1))
    mine = jnp.where(
        quarter == 0, folded[0],
        jnp.where(quarter == 1, folded[1], jnp.where(quarter == 2, folded[2], folded[3])),
    )
    mine = mine + pltpu.roll(mine, 4, 0)
    mine = mine + pltpu.roll(mine, 2, 0)
    mine = mine + pltpu.roll(mine, 1, 0)
    part_a[...] = mine[0:1]

    def a_copy(k, peer, slot):
        return pltpu.make_async_remote_copy(
            src_ref=part_a, dst_ref=recv_a.at[slot], send_sem=as_sem.at[k], recv_sem=ar_sem.at[slot],
            device_id=(peer, gy, gz), device_id_type=MESH,
        )

    def b_copy(k, peer, slot):
        return pltpu.make_async_remote_copy(
            src_ref=part_b, dst_ref=recv_b.at[slot], send_sem=bs_sem.at[k], recv_sem=br_sem.at[slot],
            device_id=(gx,) + peer, device_id_type=MESH,
        )

    def total(refs):
        while len(refs) > 1:
            refs = [refs[i] + refs[i + 1] if i + 1 < len(refs) else refs[i] for i in range(0, len(refs), 2)]
        return refs[0]

    @pl.loop(1, n_gx)
    def _(k):
        a_copy(k, lax.rem(gx + k, n_gx), gx).start()

    recv_a[gx] = mine[0:1]

    @pl.loop(1, n_gx)
    def _(k):
        src = lax.rem(gx + k, n_gx)
        a_copy(k, src, src).wait_recv()

    stage = total([recv_a[i] for i in range(n_gx)])
    part_b[...] = stage

    @pl.loop(1, plane_n)
    def _(k):
        b_copy(k, plane_peer(k), plane_me).start()

    recv_b[plane_me] = stage

    @pl.loop(1, plane_n)
    def _(k):
        py, pz = plane_peer(k)
        b_copy(k, (py, pz), py * n_gz + pz).wait_recv()

    whole = jnp.broadcast_to(total([recv_b[i] for i in range(plane_n)]), (8, BLK))
    for shift in (16, 8, 4, 2, 1):
        whole = whole + pltpu.roll(whole, shift, 1)
    m0, m1, m2, m3 = (
        jnp.broadcast_to(whole[:, 32 * q + 31 : 32 * q + 32], (8, BLK)) for q in range(4)
    )
    alpha_0 = m0 / m1
    square = alpha_0 * alpha_0
    grown = square * m2 / m0
    alpha_1 = (grown - 1.0) * m0 / (square * m3 - grown * grown * m1)
    c0 = alpha_0 + alpha_1 * grown
    c1 = alpha_0 * alpha_1

    @pl.loop(0, CX)
    def _(p):
        for yb in range(HALF // 8):
            a = v0[1 + p, pl.ds(TOP + 8 * yb, 8), :]
            b = v1[1 + p, pl.ds(TOP + 8 * yb, 8), :]
            c = v2[p, pl.ds(8 * yb, 8), :]
            x_out[p, pl.ds(8 * yb, 8), :] = c0 * a - c1 * b
            r_out[p, pl.ds(8 * yb, 8), :] = a - c0 * b + c1 * c

    @pl.loop(0, n_gx - 1)
    def _(t):
        tag_copy(t, target_of(t), gx).wait_send()
        tile_copy(t, target_of(t), gx).wait_send()

    for v, at in ((v0, 0), (v1, 1)):
        for copy, sends, _ in halo(v, at):
            @pl.when(sends)
            def _():
                copy().wait_send()

    @pl.loop(1, n_gx)
    def _(k):
        a_copy(k, lax.rem(gx + k, n_gx), gx).wait_send()

    @pl.loop(1, plane_n)
    def _(k):
        b_copy(k, plane_peer(k), plane_me).wait_send()


def per_device(sizes, face_blocks, owner_rank, owner_tile, live_count, right_side, diagonal):
    n_gx, n_gy, n_gz = sizes
    plane_n = n_gy * n_gz
    box = (CX, HALF, BLK)
    padded = (CX + 2, HALF + 2 * TOP, BLK)
    vmem = pl.BlockSpec(memory_space=pltpu.VMEM)
    hbm = pl.BlockSpec(memory_space=pltpu.HBM)
    dma, scratch = pltpu.SemaphoreType.DMA, pltpu.VMEM
    return pl.pallas_call(
        functools.partial(body, n_gx, n_gy, n_gz),
        out_shape=(jax.ShapeDtypeStruct(box, F32), jax.ShapeDtypeStruct(box, F32)),
        in_specs=[hbm] * 6,
        out_specs=(vmem, vmem),
        scratch_shapes=[
            pltpu.SMEM((1,), jnp.int32),
            pltpu.SMEM((NB,), jnp.int32),
            pltpu.SMEM((NB,), jnp.int32),
            pltpu.SMEM((NB,), jnp.int32),
            scratch((NB, BLK * BLK), F32),
            scratch((NB + 1, HALF, BLK), F32),
            scratch((2 * BLK, BLK), jnp.bfloat16),
            scratch((n_gx, HALF, BLK), F32),
            scratch((n_gx, HALF, BLK), F32),
            scratch((n_gx, 1, BLK), F32),
            scratch((n_gx, 1, BLK), F32),
            scratch(padded, F32),
            scratch(padded, F32),
            scratch(box, F32),
            scratch(box, F32),
            scratch((2, 2, CX, BLK), F32),
            scratch((2, 2, CX, BLK), F32),
            scratch((2, 2, 8, BLK), F32),
            scratch((2, 2, 8, BLK), F32),
            scratch((1, BLK), F32),
            scratch((1, BLK), F32),
            scratch((n_gx, 1, BLK), F32),
            scratch((plane_n, 1, BLK), F32),
            dma((9,)),
            dma((n_gx,)), dma((n_gx,)), dma((n_gx,)), dma((n_gx,)),
            dma((2, 6)), dma((2, 6)),
            dma((n_gx,)), dma((n_gx,)), dma((plane_n,)), dma((plane_n,)),
        ],
        compiler_params=pltpu.CompilerParams(
            collective_id=0, has_side_effects=True, vmem_limit_bytes=55_200_000
        ),
    )(
        live_count.reshape(1), owner_rank.reshape(NB), owner_tile.reshape(NB),
        face_blocks.reshape(NB, BLK * BLK), right_side, diagonal,
    )


def solution(mesh):
    sizes = (mesh.shape["gx"], mesh.shape["gy"], mesh.shape["gz"])
    return jax.shard_map(
        functools.partial(per_device, sizes),
        mesh=mesh,
        in_specs=(
            P("gx", "gy", "gz", None, None),
            P("gx", "gy", "gz", None, None),
            P("gx", "gy", "gz", None),
            P("gx", "gy", "gz"),
            P("gx", "gy", "gz"),
            P("gx", "gy", "gz"),
        ),
        out_specs=(P("gx", "gy", "gz"), P("gx", "gy", "gz")),
        check_vma=False,
    )
```

```python
import functools

import jax
import jax.numpy as jnp
from jax import lax
from jax.experimental import pallas as pl
from jax.experimental.pallas import tpu as pltpu
from jax.sharding import PartitionSpec as P

NB = 24
BLK = 128
HALF = BLK // 2
CX = 16
F32 = jnp.float32
MESH = pl.DeviceIdType.MESH
SHIFT = 6.5
TOP = 8


def ring_offsets(n, d):
    return tuple(sorted({d % n, -d % n} - {0}))


def body(
    n_gx, n_gy, n_gz,
    count_hbm, rank_hbm, tile_hbm, face_ref, rhs_ref, diag_ref,
    x_out, r_out,
    count_ref, rank_ref, tile_ref, live_rank, face, rows, pair, sbuf, rbuf, stag, rtag,
    v0, v1, v2, diag, ysend, yrecv, zsend, zrecv,
    part_a, part_b, recv_a, recv_b,
    known, in_sem, s_sem, r_sem, st_sem, rt_sem, hs_sem, hr_sem,
    as_sem, ar_sem, bs_sem, br_sem,
):
    gx, gy, gz = lax.axis_index("gx"), lax.axis_index("gy"), lax.axis_index("gz")
    chips = n_gx // 2
    chip, core = gx // 2, gx % 2
    plane_n = n_gy * n_gz
    plane_me = gy * n_gz + gz
    barrier = pltpu.get_barrier_semaphore()

    def step_chip(t):
        j = t // 2
        return (1 - 2 * (j % 2)) * (chips // 2 - (j + 1) // 2)

    def target_of(t):
        return lax.rem(chip + step_chip(t) + chips, chips) * 2 + lax.rem(core + 1 + t, 2)

    def source_of(t):
        return lax.rem(chip - step_chip(t) + chips, chips) * 2 + lax.rem(core + 1 + t, 2)

    zrecv[...] = jnp.zeros_like(zrecv)
    yrecv[...] = jnp.zeros_like(yrecv)

    near_y, near_z = ring_offsets(n_gy, 1), ring_offsets(n_gz, 1)
    far_z = ring_offsets(n_gz, 2) if n_gz > 4 else ()

    def along_y(k):
        return (gx, lax.rem(gy + k, n_gy), gz)

    def along_z(k):
        return (gx, gy, lax.rem(gz + k, n_gz))

    def tell(sem, peer):
        pl.semaphore_signal(sem, inc=1, device_id=peer, device_id_type=MESH)

    for t in range(n_gx - 1):
        tell(barrier, (target_of(t), gy, gz))
    for k in near_y:
        tell(barrier, along_y(k))
    for k in near_z:
        tell(barrier, along_z(k))

    small_copies = [
        pltpu.make_async_copy(src, dst, in_sem.at[6 + i])
        for i, (src, dst) in enumerate(
            ((count_hbm, count_ref), (rank_hbm, rank_ref), (tile_hbm, tile_ref))
        )
    ]
    for c in small_copies:
        c.start()
    pieces = 4
    width = face.shape[1] // pieces
    face_copies = [
        pltpu.make_async_copy(
            face_ref.at[:, pl.ds(i * width, width)], face.at[:, pl.ds(i * width, width)], in_sem.at[i]
        )
        for i in range(pieces)
    ]
    for c in face_copies:
        c.start()
    rhs_copy = pltpu.make_async_copy(
        rhs_ref, v0.at[pl.ds(1, CX), pl.ds(TOP, HALF), :], in_sem.at[pieces]
    )
    rhs_copy.start()
    diag_copy = pltpu.make_async_copy(diag_ref, diag, in_sem.at[pieces + 1])
    diag_copy.start()

    def plane_peer(k):
        q = lax.rem(plane_me + k, plane_n)
        return q // n_gz, lax.rem(q, n_gz)

    lane = lax.broadcasted_iota(jnp.int32, (8, BLK), 1)
    k_at = lax.broadcasted_iota(jnp.int32, (2 * BLK, BLK), 0)
    c_at = lax.broadcasted_iota(jnp.int32, (2 * BLK, BLK), 1)
    hit = (k_at // BLK == c_at // HALF) & ((k_at % BLK) // 2 == c_at % HALF)
    pair[...] = jnp.where(hit, 0.25, 0.0).astype(jnp.bfloat16)
    rows[NB] = jnp.zeros((HALF, BLK), F32)
    by_row = rows.reshape((NB + 1) * HALF, BLK)
    for c in small_copies:
        c.wait()
    count = count_ref[0]
    for s in range(NB):
        live_rank[s] = jnp.where(s < count, rank_ref[s], -1)

    @pl.when(gx == 0)
    def _():
        for v in (v0, v1):
            v[0, pl.ds(TOP, HALF), :] = jnp.zeros((HALF, BLK), F32)

    @pl.when(gx == n_gx - 1)
    def _():
        for v in (v0, v1):
            v[CX + 1, pl.ds(TOP, HALF), :] = jnp.zeros((HALF, BLK), F32)

    per = HALF // pieces
    for i in range(pieces):
        face_copies[i].wait()

        @pl.loop(0, per // 4)
        def _(r4):
            for u in range(4):
                r = i * per + r4 * 4 + u
                at = pl.multiple_of(r * 2 * BLK, 2 * BLK)
                both = face[:, pl.ds(at, BLK)] + face[:, pl.ds(at + BLK, BLK)]
                for g in range(NB // 8):
                    by_row[pl.ds(g * 8 * HALF + r, 8, stride=HALF), :] = both[g * 8 : g * 8 + 8]

    pl.semaphore_wait(barrier, n_gx - 1 + len(near_y) + len(near_z))
    for k in near_y:
        tell(known.at[0], along_y(k))
    for k in near_z:
        tell(known.at[0], along_z(k))

    def packed(tgt):
        i0, i1 = jnp.int32(NB), jnp.int32(NB)
        l0, l1 = jnp.int32(0), jnp.int32(0)
        for s in range(NB):
            named = live_rank[s] == tgt
            label = tile_ref[s] + 1
            free = i0 == NB
            first = named & free
            second = named & jnp.logical_not(free)
            i1 = jnp.where(second, s, i1)
            l1 = jnp.where(second, label, l1)
            i0 = jnp.where(first, s, i0)
            l0 = jnp.where(first, label, l0)
        a = rows[i0]
        b = rows[i1]
        w = jnp.concatenate([a, b], axis=1)
        hi = w.astype(jnp.bfloat16)
        rest = w - hi.astype(F32)
        mid = rest.astype(jnp.bfloat16)
        low = (rest - mid.astype(F32)).astype(jnp.bfloat16)
        s = pair[...]
        o = jnp.dot(hi, s, preferred_element_type=F32)
        o = o + jnp.dot(mid, s, preferred_element_type=F32)
        o = o + jnp.dot(low, s, preferred_element_type=F32)
        tag = jnp.where(lane[0:1] < HALF, l0, l1).astype(F32)
        return o, tag

    def tile_copy(t, tgt, slot):
        return pltpu.make_async_remote_copy(
            src_ref=sbuf.at[t], dst_ref=rbuf.at[slot], send_sem=s_sem.at[t], recv_sem=r_sem.at[slot],
            device_id=(tgt, gy, gz), device_id_type=MESH,
        )

    def tag_copy(t, tgt, slot):
        return pltpu.make_async_remote_copy(
            src_ref=stag.at[t], dst_ref=rtag.at[slot], send_sem=st_sem.at[t], recv_sem=rt_sem.at[slot],
            device_id=(tgt, gy, gz), device_id_type=MESH,
        )

    last = n_gx - 1

    @pl.loop(0, n_gx)
    def _(t):
        tgt = target_of(t)
        o, tag = packed(tgt)

        @pl.when(t < last)
        def _():
            stag[t] = tag
            sbuf[t] = o
            tag_copy(t, tgt, gx).start()
            tile_copy(t, tgt, gx).start()

        @pl.when(t == last)
        def _():
            rtag[gx] = tag
            rbuf[gx] = o

    def add_tiles(tile, tag):
        swapped = pltpu.roll(tile, HALF, 1)
        tag = jnp.broadcast_to(tag, (8, BLK))
        tag_swapped = pltpu.roll(tag, HALF, 1)[0:1]
        tag = tag[0:1]
        want = (lane[0:1] // HALF + 1).astype(F32)

        @pl.loop(0, CX // 4)
        def _(x4):
            for u in range(4):
                x = x4 * 4 + u
                here = want + (2 * x).astype(F32)
                m = jnp.broadcast_to(tag == here, (HALF, BLK))
                ms = jnp.broadcast_to(tag_swapped == here, (HALF, BLK))
                more = jnp.where(m, tile, 0.0) + jnp.where(ms, swapped, 0.0)
                v0[1 + x, pl.ds(TOP, HALF), :] = v0[1 + x, pl.ds(TOP, HALF), :] + more

    rhs_copy.wait()
    pl.semaphore_wait(known.at[0], len(near_y) + len(near_z))
    for k in far_z:
        tell(known.at[1], along_z(k))

    @pl.loop(0, n_gx)
    def _(i):
        t = lax.rem(i + last, n_gx)
        src = source_of(t)

        @pl.when(t < last)
        def _():
            tag_copy(t, src, src).wait_recv()
            tile_copy(t, src, src).wait_recv()

        @pl.when(i == n_gx // 2)
        def _():
            if far_z:
                pl.semaphore_wait(known.at[1], len(far_z))
            for k in range(1, n_gy):
                tell(known.at[2], along_y(k))

        add_tiles(rbuf[src], rtag[src])

    if n_gy > 1:
        pl.semaphore_wait(known.at[2], n_gy - 1)
    diag_copy.wait()

    def total(refs):
        while len(refs) > 1:
            refs = [refs[i] + refs[i + 1] if i + 1 < len(refs) else refs[i] for i in range(0, len(refs), 2)]
        return refs[0]

    ends = (lane == 0) | (lane == BLK - 1)
    even = lane % 2 == 0
    inner = pl.ds(TOP, HALF)

    def halo(v, at):
        def x_down():
            return pltpu.make_async_remote_copy(
                src_ref=v.at[1, inner, :], dst_ref=v.at[CX + 1, inner, :],
                send_sem=hs_sem.at[at, 0], recv_sem=hr_sem.at[at, 0],
                device_id=(gx - 1, gy, gz), device_id_type=MESH,
            )

        def x_up():
            return pltpu.make_async_remote_copy(
                src_ref=v.at[CX, inner, :], dst_ref=v.at[0, inner, :],
                send_sem=hs_sem.at[at, 1], recv_sem=hr_sem.at[at, 1],
                device_id=(gx + 1, gy, gz), device_id_type=MESH,
            )

        def y_down():
            return pltpu.make_async_remote_copy(
                src_ref=ysend.at[at, 0], dst_ref=yrecv.at[at, 0],
                send_sem=hs_sem.at[at, 2], recv_sem=hr_sem.at[at, 2],
                device_id=(gx, gy - 1, gz), device_id_type=MESH,
            )

        def y_up():
            return pltpu.make_async_remote_copy(
                src_ref=ysend.at[at, 1], dst_ref=yrecv.at[at, 1],
                send_sem=hs_sem.at[at, 3], recv_sem=hr_sem.at[at, 3],
                device_id=(gx, gy + 1, gz), device_id_type=MESH,
            )

        def z_down():
            return pltpu.make_async_remote_copy(
                src_ref=zsend.at[at, 0], dst_ref=zrecv.at[at, 0],
                send_sem=hs_sem.at[at, 4], recv_sem=hr_sem.at[at, 4],
                device_id=(gx, gy, gz - 1), device_id_type=MESH,
            )

        def z_up():
            return pltpu.make_async_remote_copy(
                src_ref=zsend.at[at, 1], dst_ref=zrecv.at[at, 1],
                send_sem=hs_sem.at[at, 5], recv_sem=hr_sem.at[at, 5],
                device_id=(gx, gy, gz + 1), device_id_type=MESH,
            )

        return (
            (x_down, gx > 0, gx < n_gx - 1),
            (x_up, gx < n_gx - 1, gx > 0),
            (y_down, gy > 0, gy < n_gy - 1),
            (y_up, gy < n_gy - 1, gy > 0),
            (z_down, gz > 0, gz < n_gz - 1),
            (z_up, gz < n_gz - 1, gz > 0),
        )

    def send_faces(v, at):
        faces = halo(v, at)

        def go(which):
            for copy, sends, _ in which:
                @pl.when(sends)
                def _():
                    copy().start()

        go(faces[:2])
        for p in range(CX):
            ysend[at, 0, pl.ds(p, 1), :] = v[1 + p, pl.ds(TOP, 1), :]
            ysend[at, 1, pl.ds(p, 1), :] = v[1 + p, pl.ds(TOP + HALF - 1, 1), :]
        go(faces[2:4])

        parts = [[], []]
        for p in range(CX):
            for yb in range(HALF // 8):
                c = jnp.where(ends, v[1 + p, pl.ds(TOP + 8 * yb, 8), :], 0.0)
                parts[p % 2].append(pltpu.roll(c, 16 * yb + p, 1) if 16 * yb + p else c)
        v_even, v_odd = total(parts[0]), total(parts[1])
        zsend[at, 0] = jnp.where(even, v_even, v_odd)
        zsend[at, 1] = jnp.where(even, v_odd, v_even)
        go(faces[4:])

    def take_faces(v, at):
        for copy, _, receives in halo(v, at):
            @pl.when(receives)
            def _():
                copy().wait_recv()
        for p in range(CX):
            v[1 + p, pl.ds(TOP + HALF, 1), :] = yrecv[at, 0, pl.ds(p, 1), :]
            v[1 + p, pl.ds(TOP - 1, 1), :] = yrecv[at, 1, pl.ds(p, 1), :]
        right, left = zrecv[at, 0], zrecv[at, 1]
        return jnp.where(even, right, left), jnp.where(even, left, right)

    def apply(v, at, visit, sums):
        sides = take_faces(v, at)

        step = 4

        def planes(i, sums):
            base = i * step
            here = [pltpu.roll(side, lax.rem(BLK - base, BLK), 1) for side in sides]
            for u in range(step):
                p = base + u
                for yb in range(HALF // 8):
                    row, k = TOP + 8 * yb, 16 * yb + u
                    h = pltpu.roll(here[u % 2], BLK - k, 1) if k else here[0]
                    c = v[1 + p, pl.ds(row, 8), :]
                    near = v[p, pl.ds(row, 8), :] + v[2 + p, pl.ds(row, 8), :]
                    near = near + (v[1 + p, pl.ds(row - 1, 8), :] + v[1 + p, pl.ds(row + 1, 8), :])
                    z_low = pltpu.roll(jnp.where(lane == BLK - 1, h, c), 1, 1)
                    z_high = pltpu.roll(jnp.where(lane == 0, h, c), BLK - 1, 1)
                    near = near + (z_low + z_high)
                    image = (diag[p, pl.ds(8 * yb, 8), :] + (6.0 - SHIFT)) * c - near
                    sums = visit(p, yb, c, image, sums)
            return sums

        return lax.fori_loop(0, CX // step, planes, sums)

    zero = jnp.zeros((8, BLK), F32)

    def visit_1(p, yb, c, image, sums):
        v1[1 + p, pl.ds(TOP + 8 * yb, 8), :] = image
        return sums[0] + c * c, sums[1] + c * image, sums[2] + image * image

    def visit_2(p, yb, c, image, sums):
        v2[p, pl.ds(8 * yb, 8), :] = image
        return sums + c * image

    send_faces(v0, 0)
    m0, m1, m2 = apply(v0, 0, visit_1, (zero, zero, zero))
    send_faces(v1, 1)
    m3 = apply(v1, 1, visit_2, zero)

    quarter = lane // 32
    folded = []
    for m in (m0, m1, m2, m3):
        m = m + pltpu.roll(m, 64, 1)
        folded.append(m + pltpu.roll(m, 32, 1))
    mine = jnp.where(
        quarter == 0, folded[0],
        jnp.where(quarter == 1, folded[1], jnp.where(quarter == 2, folded[2], folded[3])),
    )
    mine = mine + pltpu.roll(mine, 4, 0)
    mine = mine + pltpu.roll(mine, 2, 0)
    mine = mine + pltpu.roll(mine, 1, 0)
    part_a[...] = mine[0:1]

    def a_copy(k, peer, slot):
        return pltpu.make_async_remote_copy(
            src_ref=part_a, dst_ref=recv_a.at[slot], send_sem=as_sem.at[k], recv_sem=ar_sem.at[slot],
            device_id=(peer, gy, gz), device_id_type=MESH,
        )

    def b_copy(k, peer, slot):
        return pltpu.make_async_remote_copy(
            src_ref=part_b, dst_ref=recv_b.at[slot], send_sem=bs_sem.at[k], recv_sem=br_sem.at[slot],
            device_id=(gx,) + peer, device_id_type=MESH,
        )

    @pl.loop(1, n_gx)
    def _(k):
        a_copy(k, lax.rem(gx + k, n_gx), gx).start()

    recv_a[gx] = mine[0:1]

    @pl.loop(0, n_gx - 1)
    def _(t):
        tag_copy(t, target_of(t), gx).wait_send()
        tile_copy(t, target_of(t), gx).wait_send()

    for v, at in ((v0, 0), (v1, 1)):
        for copy, sends, _ in halo(v, at):
            @pl.when(sends)
            def _():
                copy().wait_send()

    @pl.loop(1, n_gx)
    def _(k):
        src = lax.rem(gx + k, n_gx)
        a_copy(k, src, src).wait_recv()

    stage = total([recv_a[i] for i in range(n_gx)])
    part_b[...] = stage

    @pl.loop(1, plane_n)
    def _(k):
        b_copy(k, plane_peer(k), plane_me).start()

    recv_b[plane_me] = stage

    @pl.loop(1, n_gx)
    def _(k):
        a_copy(k, lax.rem(gx + k, n_gx), gx).wait_send()

    @pl.loop(1, plane_n)
    def _(k):
        b_copy(k, plane_peer(k), plane_me).wait_send()

    @pl.loop(1, plane_n)
    def _(k):
        py, pz = plane_peer(k)
        b_copy(k, (py, pz), py * n_gz + pz).wait_recv()

    whole = jnp.broadcast_to(total([recv_b[i] for i in range(plane_n)]), (8, BLK))
    for shift in (16, 8, 4, 2, 1):
        whole = whole + pltpu.roll(whole, shift, 1)
    m0, m1, m2, m3 = (
        jnp.broadcast_to(whole[:, 32 * q + 31 : 32 * q + 32], (8, BLK)) for q in range(4)
    )
    e = m1 / m0
    a0 = 1.0 / (SHIFT + e)
    s = m2 - e * m1
    grow = a0 * s / m0
    a1 = 1.0 / (SHIFT + (m3 - 2.0 * e * m2 + e * e * m1) / s - grow)
    b0 = a0 * grow
    x0 = a0 + a1 * (b0 + a0 * e)
    x1 = a1 * a0
    r0 = a0 * e * (1.0 - a1 * SHIFT) - a1 * b0 * SHIFT
    r1 = a0 * (a1 * (SHIFT - e) - 1.0) - a1 * b0

    @pl.loop(0, CX)
    def _(p):
        for yb in range(HALF // 8):
            a = v0[1 + p, pl.ds(TOP + 8 * yb, 8), :]
            b = v1[1 + p, pl.ds(TOP + 8 * yb, 8), :]
            c = v2[p, pl.ds(8 * yb, 8), :]
            x_out[p, pl.ds(8 * yb, 8), :] = x0 * a - x1 * b
            r_out[p, pl.ds(8 * yb, 8), :] = r0 * a + (r1 * b + x1 * c)


def per_device(sizes, face_blocks, owner_rank, owner_tile, live_count, right_side, diagonal):
    n_gx, n_gy, n_gz = sizes
    plane_n = n_gy * n_gz
    box = (CX, HALF, BLK)
    padded = (CX + 2, HALF + 2 * TOP, BLK)
    vmem = pl.BlockSpec(memory_space=pltpu.VMEM)
    hbm = pl.BlockSpec(memory_space=pltpu.HBM)
    dma, scratch = pltpu.SemaphoreType.DMA, pltpu.VMEM
    return pl.pallas_call(
        functools.partial(body, n_gx, n_gy, n_gz),
        out_shape=(jax.ShapeDtypeStruct(box, F32), jax.ShapeDtypeStruct(box, F32)),
        in_specs=[hbm] * 6,
        out_specs=(vmem, vmem),
        scratch_shapes=[
            pltpu.SMEM((1,), jnp.int32),
            pltpu.SMEM((NB,), jnp.int32),
            pltpu.SMEM((NB,), jnp.int32),
            pltpu.SMEM((NB,), jnp.int32),
            scratch((NB, BLK * BLK), F32),
            scratch((NB + 1, HALF, BLK), F32),
            scratch((2 * BLK, BLK), jnp.bfloat16),
            scratch((n_gx, HALF, BLK), F32),
            scratch((n_gx, HALF, BLK), F32),
            scratch((n_gx, 1, BLK), F32),
            scratch((n_gx, 1, BLK), F32),
            scratch(padded, F32),
            scratch(padded, F32),
            scratch(box, F32),
            scratch(box, F32),
            scratch((2, 2, CX, BLK), F32),
            scratch((2, 2, CX, BLK), F32),
            scratch((2, 2, 8, BLK), F32),
            scratch((2, 2, 8, BLK), F32),
            scratch((1, BLK), F32),
            scratch((1, BLK), F32),
            scratch((n_gx, 1, BLK), F32),
            scratch((plane_n, 1, BLK), F32),
            pltpu.SemaphoreType.REGULAR((3,)),
            dma((9,)),
            dma((n_gx,)), dma((n_gx,)), dma((n_gx,)), dma((n_gx,)),
            dma((2, 6)), dma((2, 6)),
            dma((n_gx,)), dma((n_gx,)), dma((plane_n,)), dma((plane_n,)),
        ],
        compiler_params=pltpu.CompilerParams(
            collective_id=0, has_side_effects=True, vmem_limit_bytes=55_200_000
        ),
    )(
        live_count.reshape(1), owner_rank.reshape(NB), owner_tile.reshape(NB),
        face_blocks.reshape(NB, BLK * BLK), right_side, diagonal,
    )


def solution(mesh):
    sizes = (mesh.shape["gx"], mesh.shape["gy"], mesh.shape["gz"])
    return jax.shard_map(
        functools.partial(per_device, sizes),
        mesh=mesh,
        in_specs=(
            P("gx", "gy", "gz", None, None),
            P("gx", "gy", "gz", None, None),
            P("gx", "gy", "gz", None),
            P("gx", "gy", "gz"),
            P("gx", "gy", "gz"),
            P("gx", "gy", "gz"),
        ),
        out_specs=(P("gx", "gy", "gz"), P("gx", "gy", "gz")),
        check_vma=False,
    )
```

```python
import functools

import jax
import jax.numpy as jnp
from jax import lax
from jax.experimental import pallas as pl
from jax.experimental.pallas import tpu as pltpu
from jax.sharding import PartitionSpec as P

NB = 24
BLK = 128
HALF = BLK // 2
CX = 16
F32 = jnp.float32
MESH = pl.DeviceIdType.MESH
SHIFT = 6.5
TOP = 16
TWO = 2


def ring_offsets(n, d):
    return tuple(sorted({d % n, -d % n} - {0}))


def body(
    n_gx, n_gy, n_gz,
    small_hbm, face_ref, rhs_ref, diag_ref,
    x_out, r_out,
    small, live_rank, face, rows, pair, sbuf, rbuf, stag, rtag,
    v0, v1, v2, diag, ysend, yrecv, zsend, zrecv, xy, xz, yz,
    dysend, dyrecv, dzsend, dzrecv,
    part_a, part_b, recv_a, recv_b,
    known, in_sem, s_sem, r_sem, st_sem, rt_sem, hs_sem, hr_sem, ds_sem, dr_sem,
    as_sem, ar_sem, bs_sem, br_sem,
):
    gx, gy, gz = lax.axis_index("gx"), lax.axis_index("gy"), lax.axis_index("gz")
    chips = n_gx // 2
    chip, core = gx // 2, gx % 2
    plane_n = n_gy * n_gz
    plane_me = gy * n_gz + gz
    barrier = pltpu.get_barrier_semaphore()

    def step_chip(t):
        j = t // 2
        return (1 - 2 * (j % 2)) * (chips // 2 - (j + 1) // 2)

    def target_of(t):
        return lax.rem(chip + step_chip(t) + chips, chips) * 2 + lax.rem(core + 1 + t, 2)

    def source_of(t):
        return lax.rem(chip - step_chip(t) + chips, chips) * 2 + lax.rem(core + 1 + t, 2)

    for edge in (zrecv, yrecv, xy, xz, yz, dyrecv):
        edge[...] = jnp.zeros_like(edge)

    near_y, near_z = ring_offsets(n_gy, 1), ring_offsets(n_gz, 1)
    far_z = ring_offsets(n_gz, 2) if n_gz > 4 else ()

    def along_y(k):
        return (gx, lax.rem(gy + k, n_gy), gz)

    def along_z(k):
        return (gx, gy, lax.rem(gz + k, n_gz))

    def tell(sem, peer):
        pl.semaphore_signal(sem, inc=1, device_id=peer, device_id_type=MESH)

    for t in range(n_gx - 1):
        tell(barrier, (target_of(t), gy, gz))
    for k in near_y:
        tell(barrier, along_y(k))
    for k in near_z:
        tell(barrier, along_z(k))

    small_copies = [pltpu.make_async_copy(small_hbm, small, in_sem.at[6])]
    for c in small_copies:
        c.start()
    pieces = 4
    width = face.shape[1] // pieces
    face_copies = [
        pltpu.make_async_copy(
            face_ref.at[:, pl.ds(i * width, width)], face.at[:, pl.ds(i * width, width)], in_sem.at[i]
        )
        for i in range(pieces)
    ]
    for c in face_copies:
        c.start()
    rhs_copy = pltpu.make_async_copy(
        rhs_ref, v0.at[pl.ds(TWO, CX), pl.ds(TOP, HALF), :], in_sem.at[pieces]
    )
    rhs_copy.start()
    diag_copy = pltpu.make_async_copy(
        diag_ref, diag.at[pl.ds(TWO, CX), pl.ds(TOP, HALF), :], in_sem.at[pieces + 1]
    )
    diag_copy.start()

    def out_in(t, n):
        return (1 - 2 * (t % 2)) * (n // 2 - (t + 1) // 2)

    def plane_peer(t):
        py = lax.rem(gy + out_in(t % n_gy, n_gy) + n_gy, n_gy)
        return py, lax.rem(gz + out_in(t // n_gy, n_gz) + n_gz, n_gz)

    lane = lax.broadcasted_iota(jnp.int32, (8, BLK), 1)
    k_at = lax.broadcasted_iota(jnp.int32, (2 * BLK, BLK), 0)
    c_at = lax.broadcasted_iota(jnp.int32, (2 * BLK, BLK), 1)
    hit = (k_at // BLK == c_at // HALF) & ((k_at % BLK) // 2 == c_at % HALF)
    pair[...] = jnp.where(hit, 0.25, 0.0).astype(jnp.bfloat16)
    rows[NB] = jnp.zeros((HALF, BLK), F32)
    by_row = rows.reshape((NB + 1) * HALF, BLK)
    inner = pl.ds(TOP, HALF)

    def clear_plane(v, at):
        v[at, inner, :] = jnp.zeros((HALF, BLK), F32)

    @pl.when(gx == 0)
    def _():
        clear_plane(v0, 1)

    @pl.when(gx == n_gx - 1)
    def _():
        clear_plane(v0, TWO + CX)

    per = HALF // pieces
    for i in range(pieces):
        face_copies[i].wait()

        @pl.loop(0, per // 4)
        def _(r4):
            for u in range(4):
                r = i * per + r4 * 4 + u
                at = pl.multiple_of(r * 2 * BLK, 2 * BLK)
                both = face[:, pl.ds(at, BLK)] + face[:, pl.ds(at + BLK, BLK)]
                for g in range(NB // 8):
                    by_row[pl.ds(g * 8 * HALF + r, 8, stride=HALF), :] = both[g * 8 : g * 8 + 8]

    for c in small_copies:
        c.wait()
    count = small[2 * NB]
    for s in range(NB):
        live_rank[s] = jnp.where(s < count, small[s], -1)

    pl.semaphore_wait(barrier, n_gx - 1 + len(near_y) + len(near_z))
    for k in near_y:
        tell(known.at[0], along_y(k))
    for k in near_z:
        tell(known.at[0], along_z(k))

    def packed(tgt):
        i0, i1 = jnp.int32(NB), jnp.int32(NB)
        l0, l1 = jnp.int32(0), jnp.int32(0)
        for s in range(NB):
            named = live_rank[s] == tgt
            label = small[NB + s] + 1
            free = i0 == NB
            first = named & free
            second = named & jnp.logical_not(free)
            i1 = jnp.where(second, s, i1)
            l1 = jnp.where(second, label, l1)
            i0 = jnp.where(first, s, i0)
            l0 = jnp.where(first, label, l0)
        a = rows[i0]
        b = rows[i1]
        w = jnp.concatenate([a, b], axis=1)
        hi = w.astype(jnp.bfloat16)
        rest = w - hi.astype(F32)
        mid = rest.astype(jnp.bfloat16)
        low = (rest - mid.astype(F32)).astype(jnp.bfloat16)
        s = pair[...]
        o = jnp.dot(hi, s, preferred_element_type=F32)
        o = o + jnp.dot(mid, s, preferred_element_type=F32)
        o = o + jnp.dot(low, s, preferred_element_type=F32)
        tag = jnp.where(lane[0:1] < HALF, l0, l1).astype(F32)
        return o, tag

    def tile_copy(t, tgt, slot):
        return pltpu.make_async_remote_copy(
            src_ref=sbuf.at[t], dst_ref=rbuf.at[slot], send_sem=s_sem.at[t], recv_sem=r_sem.at[slot],
            device_id=(tgt, gy, gz), device_id_type=MESH,
        )

    def tag_copy(t, tgt, slot):
        return pltpu.make_async_remote_copy(
            src_ref=stag.at[t], dst_ref=rtag.at[slot], send_sem=st_sem.at[t], recv_sem=rt_sem.at[slot],
            device_id=(tgt, gy, gz), device_id_type=MESH,
        )

    last = n_gx - 1

    @pl.loop(0, n_gx)
    def _(t):
        tgt = target_of(t)
        o, tag = packed(tgt)

        @pl.when(t < last)
        def _():
            stag[t] = tag
            sbuf[t] = o
            tag_copy(t, tgt, gx).start()
            tile_copy(t, tgt, gx).start()

        @pl.when(t == last)
        def _():
            rtag[gx] = tag
            rbuf[gx] = o

    def add_tiles(tile, tag):
        swapped = pltpu.roll(tile, HALF, 1)
        tag = jnp.broadcast_to(tag, (8, BLK))
        tag_swapped = pltpu.roll(tag, HALF, 1)[0:1]
        tag = tag[0:1]
        want = (lane[0:1] // HALF + 1).astype(F32)

        @pl.loop(0, CX // 4)
        def _(x4):
            for u in range(4):
                x = x4 * 4 + u
                here = want + (2 * x).astype(F32)
                m = jnp.broadcast_to(tag == here, (HALF, BLK))
                ms = jnp.broadcast_to(tag_swapped == here, (HALF, BLK))
                more = jnp.where(m, tile, 0.0) + jnp.where(ms, swapped, 0.0)
                v0[TWO + x, inner, :] = v0[TWO + x, inner, :] + more

    def total(refs):
        while len(refs) > 1:
            refs = [refs[i] + refs[i + 1] if i + 1 < len(refs) else refs[i] for i in range(0, len(refs), 2)]
        return refs[0]

    even = lane % 2 == 0
    fourth = lane % 4
    outer = (lane < 2) | (lane >= BLK - 2)

    def z_columns(v):
        parts = [[], [], [], []]
        for p in range(CX):
            for yb in range(HALF // 8):
                c = jnp.where(outer, v[TWO + p, pl.ds(TOP + 8 * yb, 8), :], 0.0)
                k = 16 * yb + p
                parts[p % 4].append(pltpu.roll(c, k, 1) if k else c)
        parts = [total(p) for p in parts]

        def pick(off):
            out = parts[0]
            for j in range(1, 4):
                out = jnp.where(fourth == (j + off) % 4, parts[j], out)
            return pltpu.roll(out, -off % BLK, 1) if off else out

        return pick(0), pick(1), pick(-2), pick(-1)

    def within(off):
        sends, takes = [], []
        for o, at, n in zip(off, (gx, gy, gz), (n_gx, n_gy, n_gz)):
            if o:
                sends.append(at > 0 if o < 0 else at < n - 1)
                takes.append(at < n - 1 if o < 0 else at > 0)
        return functools.reduce(jnp.logical_and, sends), functools.reduce(jnp.logical_and, takes)

    def message(off, src, dst, s_sem, r_sem):
        return pltpu.make_async_remote_copy(
            src_ref=src, dst_ref=dst, send_sem=s_sem, recv_sem=r_sem,
            device_id=(gx + off[0], gy + off[1], gz + off[2]), device_id_type=MESH,
        )

    def each(messages, s_sems, r_sems, what):
        for i, (off, src, dst) in messages:
            sends, takes = within(off)

            @pl.when(takes if what == "take" else sends)
            def _():
                m = message(off, src, dst, s_sems.at[i], r_sems.at[i])
                if what == "send":
                    m.start()
                elif what == "take":
                    m.wait_recv()
                else:
                    m.wait_send()

    ways = (-1, 1)
    diag_messages = list(enumerate(
        [((-1, 0, 0), diag.at[TWO, inner, :], diag.at[TWO + CX, inner, :]),
         ((1, 0, 0), diag.at[TWO + CX - 1, inner, :], diag.at[TWO - 1, inner, :])]
        + [((0, o, 0), dysend.at[i], dyrecv.at[i]) for i, o in enumerate(ways)]
        + [((0, 0, o), dzsend.at[i], dzrecv.at[i]) for i, o in enumerate(ways)]
    ))
    x_messages = [
        ((o, 0, 0), v0.at[src + deep, inner, :], v0.at[dst + deep, inner, :])
        for o, src, dst in ((-1, TWO, TWO + CX), (1, CX, 0))
        for deep in range(2)
    ]
    y_messages = [
        ((a, b, 0), ysend.at[j, 0, i * (CX - 1)], xy.at[i, j])
        for i, a in enumerate(ways) for j, b in enumerate(ways)
    ] + [((0, o, 0), ysend.at[i], yrecv.at[i]) for i, o in enumerate(ways)]
    z_messages = [
        ((a, 0, b), zsend.at[j, 0], xz.at[i, j])
        for i, a in enumerate(ways) for j, b in enumerate(ways)
    ] + [
        ((0, a, b), zsend.at[j, 0], yz.at[i, j])
        for i, a in enumerate(ways) for j, b in enumerate(ways)
    ] + [((0, 0, o), zsend.at[i], zrecv.at[i]) for i, o in enumerate(ways)]
    side_messages = list(enumerate(x_messages + y_messages + z_messages))
    n_x, n_y = len(x_messages), len(x_messages) + len(y_messages)

    diag_copy.wait()
    for p in range(CX):
        dysend[0, p] = diag[TWO + p, pl.ds(TOP, 1), :]
        dysend[1, p] = diag[TWO + p, pl.ds(TOP + HALF - 1, 1), :]
    first, _, _, final = z_columns(diag)
    dzsend[0] = first
    dzsend[1] = final
    each(diag_messages, ds_sem, dr_sem, "send")

    rhs_copy.wait()
    pl.semaphore_wait(known.at[0], len(near_y) + len(near_z))
    for k in far_z:
        tell(known.at[1], along_z(k))

    @pl.loop(0, n_gx)
    def _(i):
        t = lax.rem(i + last, n_gx)
        src = source_of(t)

        @pl.when(t < last)
        def _():
            tag_copy(t, src, src).wait_recv()
            tile_copy(t, src, src).wait_recv()

        @pl.when(i == n_gx // 2)
        def _():
            if far_z:
                pl.semaphore_wait(known.at[1], len(far_z))
            for k in range(1, n_gy):
                tell(known.at[2], along_y(k))

        add_tiles(rbuf[src], rtag[src])

    if n_gy > 1:
        pl.semaphore_wait(known.at[2], n_gy - 1)

    each(side_messages[:n_x], hs_sem, hr_sem, "send")
    for p in range(CX):
        for deep in range(2):
            ysend[0, deep, p] = v0[TWO + p, pl.ds(TOP + deep, 1), :]
            ysend[1, deep, p] = v0[TWO + p, pl.ds(TOP + HALF - 1 - deep, 1), :]
    each(side_messages[n_x:n_y], hs_sem, hr_sem, "send")
    z_first, z_second, z_third, z_final = z_columns(v0)
    zsend[0, 0], zsend[0, 1] = z_first, z_second
    zsend[1, 0], zsend[1, 1] = z_final, z_third
    each(side_messages[n_y:], hs_sem, hr_sem, "send")

    each(diag_messages, ds_sem, dr_sem, "take")
    each(side_messages, hs_sem, hr_sem, "take")

    low, high = pl.ds(TOP - 1, 1), pl.ds(TOP + HALF, 1)
    for p in range(CX):
        diag[TWO + p, high, :] = dyrecv[0, p]
        diag[TWO + p, low, :] = dyrecv[1, p]
        v0[TWO + p, high, :] = yrecv[0, 0, p]
        v0[TWO + p, pl.ds(TOP + HALF + 1, 1), :] = yrecv[0, 1, p]
        v0[TWO + p, low, :] = yrecv[1, 0, p]
        v0[TWO + p, pl.ds(TOP - 2, 1), :] = yrecv[1, 1, p]
    for i, plane in enumerate((TWO + CX, TWO - 1)):
        v0[plane, high, :] = xy[i, 0]
        v0[plane, low, :] = xy[i, 1]

    def sides_of(right, left):
        left = pltpu.roll(left, BLK - 1, 1)
        return jnp.where(even, right, left), jnp.where(even, left, right)

    def image_of(v, plane, row, h):
        c = v[plane, pl.ds(row, 8), :]
        near = v[plane - 1, pl.ds(row, 8), :] + v[plane + 1, pl.ds(row, 8), :]
        near = near + (v[plane, pl.ds(row - 1, 8), :] + v[plane, pl.ds(row + 1, 8), :])
        z_low = pltpu.roll(jnp.where(lane == BLK - 1, h, c), 1, 1)
        z_high = pltpu.roll(jnp.where(lane == 0, h, c), BLK - 1, 1)
        near = near + (z_low + z_high)
        return c, (diag[plane, pl.ds(row, 8), :] + (6.0 - SHIFT)) * c - near

    def turned(side, k):
        return pltpu.roll(side, BLK - k, 1) if k else side

    def apply(v, sides, below, above, visit, sums):
        step = 4

        def planes(i, sums):
            base = i * step

            def moved(pair):
                return [pltpu.roll(side, lax.rem(BLK - base, BLK), 1) for side in pair]

            here = moved(sides)
            if below is not None:
                under, over = moved(below), moved(above)
            for u in range(step):
                p = base + u
                if below is not None:
                    _, image = image_of(v, TWO + p, TOP - 8, turned(under[u % 2], BLK - 16 + u))
                    v1[TWO + p, pl.ds(TOP - 8, 8), :] = image
                    _, image = image_of(v, TWO + p, TOP + HALF, turned(over[u % 2], u))
                    v1[TWO + p, pl.ds(TOP + HALF, 8), :] = image
                for yb in range(HALF // 8):
                    h = turned(here[u % 2], 16 * yb + u)
                    c, image = image_of(v, TWO + p, TOP + 8 * yb, h)
                    sums = visit(p, yb, c, image, sums)
            return sums

        return lax.fori_loop(0, CX // step, planes, sums)

    zero = jnp.zeros((8, BLK), F32)

    def visit_1(p, yb, c, image, sums):
        v1[TWO + p, pl.ds(TOP + 8 * yb, 8), :] = image
        return sums[0] + c * c, sums[1] + c * image, sums[2] + image * image

    def visit_2(p, yb, c, image, sums):
        v2[p, pl.ds(8 * yb, 8), :] = image
        return sums + c * image

    m0, m1, m2 = apply(
        v0, sides_of(zrecv[0, 0], zrecv[1, 0]), sides_of(yz[1, 0], yz[1, 1]),
        sides_of(yz[0, 0], yz[0, 1]), visit_1, (zero, zero, zero),
    )
    ring_planes = (
        (TWO + CX, 0, sides_of(xz[0, 0], xz[0, 1])[0]),
        (TWO - 1, CX - 1, sides_of(xz[1, 0], xz[1, 1])[1]),
    )
    for plane, p, side in ring_planes:
        for yb in range(HALF // 8):
            _, image = image_of(v0, plane, TOP + 8 * yb, turned(side, 16 * yb + p))
            v1[plane, pl.ds(TOP + 8 * yb, 8), :] = image
    row = lax.broadcasted_iota(jnp.int32, (8, BLK), 0)
    in_row = lane % CX

    def ring_columns(j, own, here):
        one, two = zrecv[j, 0], zrecv[j, 1]
        x_low = jnp.where(in_row == 0, pltpu.roll(xz[1, j], BLK - 15, 1), pltpu.roll(one, 1, 1))
        x_high = jnp.where(
            in_row == CX - 1, pltpu.roll(xz[0, j], 15, 1), pltpu.roll(one, BLK - 1, 1)
        )
        down, up = pltpu.roll(one, 1, 0), pltpu.roll(one, 7, 0)
        carried = jnp.where(lane >= BLK - CX, pltpu.roll(yz[1, j], 1, 0), down)
        y_low = jnp.where(row > 0, down, pltpu.roll(carried, CX, 1))
        carried = jnp.where(lane < CX, pltpu.roll(yz[0, j], 7, 0), up)
        y_high = jnp.where(row < 7, up, pltpu.roll(carried, BLK - CX, 1))
        near = (own + two) + (x_low + x_high) + (y_low + y_high)
        return jnp.where(here, (dzrecv[j] + (6.0 - SHIFT)) * one - near, 0.0)

    right = ring_columns(0, z_final, gz < n_gz - 1)
    left = ring_columns(1, z_first, gz > 0)

    @pl.when(gx == 0)
    def _():
        clear_plane(v1, TWO - 1)

    @pl.when(gx == n_gx - 1)
    def _():
        clear_plane(v1, TWO + CX)

    @pl.when(gy == 0)
    def _():
        for p in range(CX):
            v1[TWO + p, low, :] = jnp.zeros((1, BLK), F32)

    @pl.when(gy == n_gy - 1)
    def _():
        for p in range(CX):
            v1[TWO + p, high, :] = jnp.zeros((1, BLK), F32)

    m3 = apply(v1, sides_of(right, left), None, None, visit_2, zero)

    quarter = lane // 32
    folded = []
    for m in (m0, m1, m2, m3):
        m = m + pltpu.roll(m, 64, 1)
        folded.append(m + pltpu.roll(m, 32, 1))
    mine = jnp.where(
        quarter == 0, folded[0],
        jnp.where(quarter == 1, folded[1], jnp.where(quarter == 2, folded[2], folded[3])),
    )
    mine = mine + pltpu.roll(mine, 4, 0)
    mine = mine + pltpu.roll(mine, 2, 0)
    mine = mine + pltpu.roll(mine, 1, 0)
    part_a[...] = mine[0:1]

    def a_copy(k, peer, slot):
        return pltpu.make_async_remote_copy(
            src_ref=part_a, dst_ref=recv_a.at[slot], send_sem=as_sem.at[k], recv_sem=ar_sem.at[slot],
            device_id=(peer, gy, gz), device_id_type=MESH,
        )

    def b_copy(k, peer, slot):
        return pltpu.make_async_remote_copy(
            src_ref=part_b, dst_ref=recv_b.at[slot], send_sem=bs_sem.at[k], recv_sem=br_sem.at[slot],
            device_id=(gx,) + peer, device_id_type=MESH,
        )

    @pl.loop(0, n_gx - 1)
    def _(t):
        a_copy(t, target_of(t), gx).start()

    recv_a[gx] = mine[0:1]

    @pl.loop(0, n_gx - 1)
    def _(t):
        tag_copy(t, target_of(t), gx).wait_send()
        tile_copy(t, target_of(t), gx).wait_send()

    each(diag_messages, ds_sem, dr_sem, "sent")
    each(side_messages, hs_sem, hr_sem, "sent")

    @pl.loop(0, n_gx - 1)
    def _(t):
        src = source_of(t)
        a_copy(t, src, src).wait_recv()

    stage = total([recv_a[i] for i in range(n_gx)])
    part_b[...] = stage

    @pl.loop(0, plane_n - 1)
    def _(k):
        b_copy(k, plane_peer(k), plane_me).start()

    recv_b[plane_me] = stage

    @pl.loop(0, n_gx - 1)
    def _(t):
        a_copy(t, target_of(t), gx).wait_send()

    @pl.loop(0, plane_n - 1)
    def _(k):
        b_copy(k, plane_peer(k), plane_me).wait_send()

    @pl.loop(0, plane_n - 1)
    def _(k):
        py, pz = plane_peer(k)
        b_copy(k, (py, pz), py * n_gz + pz).wait_recv()

    whole = jnp.broadcast_to(total([recv_b[i] for i in range(plane_n)]), (8, BLK))
    for shift in (16, 8, 4, 2, 1):
        whole = whole + pltpu.roll(whole, shift, 1)
    m0, m1, m2, m3 = (
        jnp.broadcast_to(whole[:, 32 * q + 31 : 32 * q + 32], (8, BLK)) for q in range(4)
    )
    e = m1 / m0
    a0 = 1.0 / (SHIFT + e)
    s = m2 - e * m1
    grow = a0 * s / m0
    a1 = 1.0 / (SHIFT + (m3 - 2.0 * e * m2 + e * e * m1) / s - grow)
    b0 = a0 * grow
    x0 = a0 + a1 * (b0 + a0 * e)
    x1 = a1 * a0
    r0 = a0 * e * (1.0 - a1 * SHIFT) - a1 * b0 * SHIFT
    r1 = a0 * (a1 * (SHIFT - e) - 1.0) - a1 * b0

    @pl.loop(0, CX)
    def _(p):
        for yb in range(HALF // 8):
            a = v0[TWO + p, pl.ds(TOP + 8 * yb, 8), :]
            b = v1[TWO + p, pl.ds(TOP + 8 * yb, 8), :]
            c = v2[p, pl.ds(8 * yb, 8), :]
            x_out[p, pl.ds(8 * yb, 8), :] = x0 * a - x1 * b
            r_out[p, pl.ds(8 * yb, 8), :] = r0 * a + (r1 * b + x1 * c)


def per_device(sizes, face_blocks, owner_rank, owner_tile, live_count, right_side, diagonal):
    n_gx, n_gy, n_gz = sizes
    plane_n = n_gy * n_gz
    box = (CX, HALF, BLK)
    padded = (CX + 2 * TWO, HALF + 2 * TOP, BLK)
    vmem = pl.BlockSpec(memory_space=pltpu.VMEM)
    hbm = pl.BlockSpec(memory_space=pltpu.HBM)
    counts = jnp.broadcast_to(live_count.reshape(1), (BLK - 2 * NB,))
    small = jnp.concatenate([owner_rank.reshape(NB), owner_tile.reshape(NB), counts])
    dma, scratch = pltpu.SemaphoreType.DMA, pltpu.VMEM
    return pl.pallas_call(
        functools.partial(body, n_gx, n_gy, n_gz),
        out_shape=(jax.ShapeDtypeStruct(box, F32), jax.ShapeDtypeStruct(box, F32)),
        in_specs=[hbm] * 4,
        out_specs=(vmem, vmem),
        scratch_shapes=[
            pltpu.SMEM((BLK,), jnp.int32),
            pltpu.SMEM((NB,), jnp.int32),
            scratch((NB, BLK * BLK), F32),
            scratch((NB + 1, HALF, BLK), F32),
            scratch((2 * BLK, BLK), jnp.bfloat16),
            scratch((n_gx, HALF, BLK), F32),
            scratch((n_gx, HALF, BLK), F32),
            scratch((n_gx, 1, BLK), F32),
            scratch((n_gx, 1, BLK), F32),
            scratch(padded, F32),
            scratch(padded, F32),
            scratch(box, F32),
            scratch(padded, F32),
            scratch((2, 2, CX, 1, BLK), F32),
            scratch((2, 2, CX, 1, BLK), F32),
            scratch((2, 2, 8, BLK), F32),
            scratch((2, 2, 8, BLK), F32),
            scratch((2, 2, 1, BLK), F32),
            scratch((2, 2, 8, BLK), F32),
            scratch((2, 2, 8, BLK), F32),
            scratch((2, CX, 1, BLK), F32),
            scratch((2, CX, 1, BLK), F32),
            scratch((2, 8, BLK), F32),
            scratch((2, 8, BLK), F32),
            scratch((1, BLK), F32),
            scratch((1, BLK), F32),
            scratch((n_gx, 1, BLK), F32),
            scratch((plane_n, 1, BLK), F32),
            pltpu.SemaphoreType.REGULAR((3,)),
            dma((9,)),
            dma((n_gx,)), dma((n_gx,)), dma((n_gx,)), dma((n_gx,)),
            dma((20,)), dma((20,)), dma((6,)), dma((6,)),
            dma((n_gx,)), dma((n_gx,)), dma((plane_n,)), dma((plane_n,)),
        ],
        compiler_params=pltpu.CompilerParams(
            collective_id=0, has_side_effects=True, vmem_limit_bytes=55_200_000
        ),
    )(
        small,
        face_blocks.reshape(NB, BLK * BLK), right_side, diagonal,
    )


def solution(mesh):
    sizes = (mesh.shape["gx"], mesh.shape["gy"], mesh.shape["gz"])
    return jax.shard_map(
        functools.partial(per_device, sizes),
        mesh=mesh,
        in_specs=(
            P("gx", "gy", "gz", None, None),
            P("gx", "gy", "gz", None, None),
            P("gx", "gy", "gz", None),
            P("gx", "gy", "gz"),
            P("gx", "gy", "gz"),
            P("gx", "gy", "gz"),
        ),
        out_specs=(P("gx", "gy", "gz"), P("gx", "gy", "gz")),
        check_vma=False,
    )
```

```python
import functools

import jax
import jax.numpy as jnp
from jax import lax
from jax.experimental import pallas as pl
from jax.experimental.pallas import tpu as pltpu
from jax.sharding import PartitionSpec as P

NB = 24
BLK = 128
HALF = BLK // 2
CX = 16
F32 = jnp.float32
MESH = pl.DeviceIdType.MESH
SHIFT = 6.5
TOP = 16
TWO = 2


def ring_offsets(n, d):
    return tuple(sorted({d % n, -d % n} - {0}))


def body(
    n_gx, n_gy, n_gz,
    small_hbm, face_ref, rhs_ref, diag_ref,
    v0_out, v1_out, v2, x0_out, x1_out, r0_out, r1_out, r2_out,
    small, live_rank, face, rows, pair, sbuf, rbuf, stag, rtag,
    v0, v1, diag, ysend, yrecv, zsend, zrecv, xy, xz, yz,
    dysend, dyrecv, dzsend, dzrecv,
    part_a, part_b, recv_a, recv_b,
    known, in_sem, s_sem, r_sem, st_sem, rt_sem, hs_sem, hr_sem, ds_sem, dr_sem,
    as_sem, ar_sem, bs_sem, br_sem,
):
    gx, gy, gz = lax.axis_index("gx"), lax.axis_index("gy"), lax.axis_index("gz")
    chips = n_gx // 2
    chip, core = gx // 2, gx % 2
    plane_n = n_gy * n_gz
    plane_me = gy * n_gz + gz
    barrier = pltpu.get_barrier_semaphore()

    def step_chip(t):
        j = t // 2
        return (1 - 2 * (j % 2)) * (chips // 2 - (j + 1) // 2)

    def target_of(t):
        return lax.rem(chip + step_chip(t) + chips, chips) * 2 + lax.rem(core + 1 + t, 2)

    def source_of(t):
        return lax.rem(chip - step_chip(t) + chips, chips) * 2 + lax.rem(core + 1 + t, 2)

    for edge in (zrecv, yrecv, xy, xz, yz, dyrecv):
        edge[...] = jnp.zeros_like(edge)

    near_y, near_z = ring_offsets(n_gy, 1), ring_offsets(n_gz, 1)
    far_z = ring_offsets(n_gz, 2) if n_gz > 4 else ()

    def along_y(k):
        return (gx, lax.rem(gy + k, n_gy), gz)

    def along_z(k):
        return (gx, gy, lax.rem(gz + k, n_gz))

    def tell(sem, peer):
        pl.semaphore_signal(sem, inc=1, device_id=peer, device_id_type=MESH)

    for t in range(n_gx - 1):
        tell(barrier, (target_of(t), gy, gz))
    for k in near_y:
        tell(barrier, along_y(k))
    for k in near_z:
        tell(barrier, along_z(k))

    small_copies = [pltpu.make_async_copy(small_hbm, small, in_sem.at[6])]
    for c in small_copies:
        c.start()
    pieces = 4
    width = face.shape[1] // pieces
    face_copies = [
        pltpu.make_async_copy(
            face_ref.at[:, pl.ds(i * width, width)], face.at[:, pl.ds(i * width, width)], in_sem.at[i]
        )
        for i in range(pieces)
    ]
    for c in face_copies:
        c.start()
    rhs_copy = pltpu.make_async_copy(
        rhs_ref, v0.at[pl.ds(TWO, CX), pl.ds(TOP, HALF), :], in_sem.at[pieces]
    )
    rhs_copy.start()
    diag_copy = pltpu.make_async_copy(
        diag_ref, diag.at[pl.ds(TWO, CX), pl.ds(TOP, HALF), :], in_sem.at[pieces + 1]
    )
    diag_copy.start()

    def out_in(t, n):
        return (1 - 2 * (t % 2)) * (n // 2 - (t + 1) // 2)

    def plane_peer(t):
        py = lax.rem(gy + out_in(t % n_gy, n_gy) + n_gy, n_gy)
        return py, lax.rem(gz + out_in(t // n_gy, n_gz) + n_gz, n_gz)

    lane = lax.broadcasted_iota(jnp.int32, (8, BLK), 1)
    k_at = lax.broadcasted_iota(jnp.int32, (2 * BLK, BLK), 0)
    c_at = lax.broadcasted_iota(jnp.int32, (2 * BLK, BLK), 1)
    hit = (k_at // BLK == c_at // HALF) & ((k_at % BLK) // 2 == c_at % HALF)
    pair[...] = jnp.where(hit, 0.25, 0.0).astype(jnp.bfloat16)
    rows[NB] = jnp.zeros((HALF, BLK), F32)
    by_row = rows.reshape((NB + 1) * HALF, BLK)
    inner = pl.ds(TOP, HALF)

    def clear_plane(v, at):
        v[at, inner, :] = jnp.zeros((HALF, BLK), F32)

    @pl.when(gx == 0)
    def _():
        clear_plane(v0, 1)

    @pl.when(gx == n_gx - 1)
    def _():
        clear_plane(v0, TWO + CX)

    per = HALF // pieces
    for i in range(pieces):
        face_copies[i].wait()

        @pl.loop(0, per // 4)
        def _(r4):
            for u in range(4):
                r = i * per + r4 * 4 + u
                at = pl.multiple_of(r * 2 * BLK, 2 * BLK)
                both = face[:, pl.ds(at, BLK)] + face[:, pl.ds(at + BLK, BLK)]
                for g in range(NB // 8):
                    by_row[pl.ds(g * 8 * HALF + r, 8, stride=HALF), :] = both[g * 8 : g * 8 + 8]

    for c in small_copies:
        c.wait()
    count = small[2 * NB]
    for s in range(NB):
        live_rank[s] = jnp.where(s < count, small[s], -1)

    pl.semaphore_wait(barrier, n_gx - 1 + len(near_y) + len(near_z))
    for k in near_y:
        tell(known.at[0], along_y(k))
    for k in near_z:
        tell(known.at[0], along_z(k))

    def packed(tgt):
        i0, i1 = jnp.int32(NB), jnp.int32(NB)
        l0, l1 = jnp.int32(0), jnp.int32(0)
        for s in range(NB):
            named = live_rank[s] == tgt
            label = small[NB + s] + 1
            free = i0 == NB
            first = named & free
            second = named & jnp.logical_not(free)
            i1 = jnp.where(second, s, i1)
            l1 = jnp.where(second, label, l1)
            i0 = jnp.where(first, s, i0)
            l0 = jnp.where(first, label, l0)
        a = rows[i0]
        b = rows[i1]
        w = jnp.concatenate([a, b], axis=1)
        hi = w.astype(jnp.bfloat16)
        rest = w - hi.astype(F32)
        mid = rest.astype(jnp.bfloat16)
        low = (rest - mid.astype(F32)).astype(jnp.bfloat16)
        s = pair[...]
        o = jnp.dot(hi, s, preferred_element_type=F32)
        o = o + jnp.dot(mid, s, preferred_element_type=F32)
        o = o + jnp.dot(low, s, preferred_element_type=F32)
        tag = jnp.where(lane[0:1] < HALF, l0, l1).astype(F32)
        return o, tag

    def tile_copy(t, tgt, slot):
        return pltpu.make_async_remote_copy(
            src_ref=sbuf.at[t], dst_ref=rbuf.at[slot], send_sem=s_sem.at[t], recv_sem=r_sem.at[slot],
            device_id=(tgt, gy, gz), device_id_type=MESH,
        )

    def tag_copy(t, tgt, slot):
        return pltpu.make_async_remote_copy(
            src_ref=stag.at[t], dst_ref=rtag.at[slot], send_sem=st_sem.at[t], recv_sem=rt_sem.at[slot],
            device_id=(tgt, gy, gz), device_id_type=MESH,
        )

    last = n_gx - 1

    @pl.loop(0, n_gx)
    def _(t):
        tgt = target_of(t)
        o, tag = packed(tgt)

        @pl.when(t < last)
        def _():
            stag[t] = tag
            sbuf[t] = o
            tag_copy(t, tgt, gx).start()
            tile_copy(t, tgt, gx).start()

        @pl.when(t == last)
        def _():
            rtag[gx] = tag
            rbuf[gx] = o

    def add_tiles(tile, tag):
        swapped = pltpu.roll(tile, HALF, 1)
        tag = jnp.broadcast_to(tag, (8, BLK))
        tag_swapped = pltpu.roll(tag, HALF, 1)[0:1]
        tag = tag[0:1]
        want = (lane[0:1] // HALF + 1).astype(F32)

        @pl.loop(0, CX // 4)
        def _(x4):
            for u in range(4):
                x = x4 * 4 + u
                here = want + (2 * x).astype(F32)
                m = jnp.broadcast_to(tag == here, (HALF, BLK))
                ms = jnp.broadcast_to(tag_swapped == here, (HALF, BLK))
                more = jnp.where(m, tile, 0.0) + jnp.where(ms, swapped, 0.0)
                v0[TWO + x, inner, :] = v0[TWO + x, inner, :] + more

    def total(refs):
        while len(refs) > 1:
            refs = [refs[i] + refs[i + 1] if i + 1 < len(refs) else refs[i] for i in range(0, len(refs), 2)]
        return refs[0]

    even = lane % 2 == 0
    fourth = lane % 4
    outer = (lane < 2) | (lane >= BLK - 2)

    def z_columns(v):
        parts = [[], [], [], []]
        for p in range(CX):
            for yb in range(HALF // 8):
                c = jnp.where(outer, v[TWO + p, pl.ds(TOP + 8 * yb, 8), :], 0.0)
                k = 16 * yb + p
                parts[p % 4].append(pltpu.roll(c, k, 1) if k else c)
        parts = [total(p) for p in parts]

        def pick(off):
            out = parts[0]
            for j in range(1, 4):
                out = jnp.where(fourth == (j + off) % 4, parts[j], out)
            return pltpu.roll(out, -off % BLK, 1) if off else out

        return pick(0), pick(1), pick(-2), pick(-1)

    def within(off):
        sends, takes = [], []
        for o, at, n in zip(off, (gx, gy, gz), (n_gx, n_gy, n_gz)):
            if o:
                sends.append(at > 0 if o < 0 else at < n - 1)
                takes.append(at < n - 1 if o < 0 else at > 0)
        return functools.reduce(jnp.logical_and, sends), functools.reduce(jnp.logical_and, takes)

    def message(off, src, dst, s_sem, r_sem):
        return pltpu.make_async_remote_copy(
            src_ref=src, dst_ref=dst, send_sem=s_sem, recv_sem=r_sem,
            device_id=(gx + off[0], gy + off[1], gz + off[2]), device_id_type=MESH,
        )

    def each(messages, s_sems, r_sems, what):
        for i, (off, src, dst) in messages:
            sends, takes = within(off)

            @pl.when(takes if what == "take" else sends)
            def _():
                m = message(off, src, dst, s_sems.at[i], r_sems.at[i])
                if what == "send":
                    m.start()
                elif what == "take":
                    m.wait_recv()
                else:
                    m.wait_send()

    ways = (-1, 1)
    diag_messages = list(enumerate(
        [((-1, 0, 0), diag.at[TWO, inner, :], diag.at[TWO + CX, inner, :]),
         ((1, 0, 0), diag.at[TWO + CX - 1, inner, :], diag.at[TWO - 1, inner, :])]
        + [((0, o, 0), dysend.at[i], dyrecv.at[i]) for i, o in enumerate(ways)]
        + [((0, 0, o), dzsend.at[i], dzrecv.at[i]) for i, o in enumerate(ways)]
    ))
    x_messages = [
        ((o, 0, 0), v0.at[src + deep, inner, :], v0.at[dst + deep, inner, :])
        for o, src, dst in ((-1, TWO, TWO + CX), (1, CX, 0))
        for deep in range(2)
    ]
    y_messages = [
        ((a, b, 0), ysend.at[j, 0, i * (CX - 1)], xy.at[i, j])
        for i, a in enumerate(ways) for j, b in enumerate(ways)
    ] + [((0, o, 0), ysend.at[i], yrecv.at[i]) for i, o in enumerate(ways)]
    z_messages = [
        ((a, 0, b), zsend.at[j, 0], xz.at[i, j])
        for i, a in enumerate(ways) for j, b in enumerate(ways)
    ] + [
        ((0, a, b), zsend.at[j, 0], yz.at[i, j])
        for i, a in enumerate(ways) for j, b in enumerate(ways)
    ] + [((0, 0, o), zsend.at[i], zrecv.at[i]) for i, o in enumerate(ways)]
    side_messages = list(enumerate(x_messages + y_messages + z_messages))
    n_x, n_y = len(x_messages), len(x_messages) + len(y_messages)

    diag_copy.wait()
    for p in range(CX):
        dysend[0, p] = diag[TWO + p, pl.ds(TOP, 1), :]
        dysend[1, p] = diag[TWO + p, pl.ds(TOP + HALF - 1, 1), :]
    first, _, _, final = z_columns(diag)
    dzsend[0] = first
    dzsend[1] = final
    each(diag_messages, ds_sem, dr_sem, "send")

    rhs_copy.wait()
    pl.semaphore_wait(known.at[0], len(near_y) + len(near_z))
    for k in far_z:
        tell(known.at[1], along_z(k))

    @pl.loop(0, n_gx)
    def _(i):
        t = lax.rem(i + last, n_gx)
        src = source_of(t)

        @pl.when(t < last)
        def _():
            tag_copy(t, src, src).wait_recv()
            tile_copy(t, src, src).wait_recv()

        @pl.when(i == n_gx // 2)
        def _():
            if far_z:
                pl.semaphore_wait(known.at[1], len(far_z))
            for k in range(1, n_gy):
                tell(known.at[2], along_y(k))

        add_tiles(rbuf[src], rtag[src])

    if n_gy > 1:
        pl.semaphore_wait(known.at[2], n_gy - 1)

    each(side_messages[:n_x], hs_sem, hr_sem, "send")
    for p in range(CX):
        for deep in range(2):
            ysend[0, deep, p] = v0[TWO + p, pl.ds(TOP + deep, 1), :]
            ysend[1, deep, p] = v0[TWO + p, pl.ds(TOP + HALF - 1 - deep, 1), :]
    each(side_messages[n_x:n_y], hs_sem, hr_sem, "send")
    z_first, z_second, z_third, z_final = z_columns(v0)
    zsend[0, 0], zsend[0, 1] = z_first, z_second
    zsend[1, 0], zsend[1, 1] = z_final, z_third
    each(side_messages[n_y:], hs_sem, hr_sem, "send")

    each(diag_messages, ds_sem, dr_sem, "take")
    each(side_messages, hs_sem, hr_sem, "take")

    low, high = pl.ds(TOP - 1, 1), pl.ds(TOP + HALF, 1)
    for p in range(CX):
        diag[TWO + p, high, :] = dyrecv[0, p]
        diag[TWO + p, low, :] = dyrecv[1, p]
        v0[TWO + p, high, :] = yrecv[0, 0, p]
        v0[TWO + p, pl.ds(TOP + HALF + 1, 1), :] = yrecv[0, 1, p]
        v0[TWO + p, low, :] = yrecv[1, 0, p]
        v0[TWO + p, pl.ds(TOP - 2, 1), :] = yrecv[1, 1, p]
    for i, plane in enumerate((TWO + CX, TWO - 1)):
        v0[plane, high, :] = xy[i, 0]
        v0[plane, low, :] = xy[i, 1]

    def sides_of(right, left):
        left = pltpu.roll(left, BLK - 1, 1)
        return jnp.where(even, right, left), jnp.where(even, left, right)

    def image_of(v, plane, row, h):
        c = v[plane, pl.ds(row, 8), :]
        near = v[plane - 1, pl.ds(row, 8), :] + v[plane + 1, pl.ds(row, 8), :]
        near = near + (v[plane, pl.ds(row - 1, 8), :] + v[plane, pl.ds(row + 1, 8), :])
        z_low = pltpu.roll(jnp.where(lane == BLK - 1, h, c), 1, 1)
        z_high = pltpu.roll(jnp.where(lane == 0, h, c), BLK - 1, 1)
        near = near + (z_low + z_high)
        return c, (diag[plane, pl.ds(row, 8), :] + (6.0 - SHIFT)) * c - near

    def turned(side, k):
        return pltpu.roll(side, BLK - k, 1) if k else side

    step = 8

    def moved(pair, base):
        return [pltpu.roll(side, lax.rem(BLK - base, BLK), 1) for side in pair]

    def apply(v, sides, visit, sums):

        def planes(i, sums):
            base = i * step
            here = moved(sides, base)
            for u in range(step):
                p = base + u
                for yb in range(HALF // 8):
                    h = turned(here[u % 2], 16 * yb + u)
                    c, image = image_of(v, TWO + p, TOP + 8 * yb, h)
                    sums = visit(p, yb, c, image, sums)
            return sums

        return lax.fori_loop(0, CX // step, planes, sums)

    zero = jnp.zeros((8, BLK), F32)

    def visit_1(p, yb, c, image, sums):
        v1[TWO + p, pl.ds(TOP + 8 * yb, 8), :] = image
        v0_out[p, pl.ds(8 * yb, 8), :] = c
        v1_out[p, pl.ds(8 * yb, 8), :] = image
        return sums[0] + c * c, sums[1] + c * image, sums[2] + image * image

    def visit_2(p, yb, c, image, sums):
        v2[p, pl.ds(8 * yb, 8), :] = image
        return sums + c * image

    m0, m1, m2 = apply(
        v0, sides_of(zrecv[0, 0], zrecv[1, 0]), visit_1, (zero, zero, zero)
    )
    below, above = sides_of(yz[1, 0], yz[1, 1]), sides_of(yz[0, 0], yz[0, 1])

    @pl.loop(0, CX // step)
    def _(i):
        base = i * step
        under, over = moved(below, base), moved(above, base)
        for u in range(step):
            p = base + u
            _, image = image_of(v0, TWO + p, TOP - 8, turned(under[u % 2], BLK - 16 + u))
            v1[TWO + p, pl.ds(TOP - 8, 8), :] = image
            _, image = image_of(v0, TWO + p, TOP + HALF, turned(over[u % 2], u))
            v1[TWO + p, pl.ds(TOP + HALF, 8), :] = image

    ring_planes = (
        (TWO + CX, 0, sides_of(xz[0, 0], xz[0, 1])[0]),
        (TWO - 1, CX - 1, sides_of(xz[1, 0], xz[1, 1])[1]),
    )
    for plane, p, side in ring_planes:
        for yb in range(HALF // 8):
            _, image = image_of(v0, plane, TOP + 8 * yb, turned(side, 16 * yb + p))
            v1[plane, pl.ds(TOP + 8 * yb, 8), :] = image
    row = lax.broadcasted_iota(jnp.int32, (8, BLK), 0)
    in_row = lane % CX

    def ring_columns(j, own, here):
        one, two = zrecv[j, 0], zrecv[j, 1]
        x_low = jnp.where(in_row == 0, pltpu.roll(xz[1, j], BLK - 15, 1), pltpu.roll(one, 1, 1))
        x_high = jnp.where(
            in_row == CX - 1, pltpu.roll(xz[0, j], 15, 1), pltpu.roll(one, BLK - 1, 1)
        )
        down, up = pltpu.roll(one, 1, 0), pltpu.roll(one, 7, 0)
        carried = jnp.where(lane >= BLK - CX, pltpu.roll(yz[1, j], 1, 0), down)
        y_low = jnp.where(row > 0, down, pltpu.roll(carried, CX, 1))
        carried = jnp.where(lane < CX, pltpu.roll(yz[0, j], 7, 0), up)
        y_high = jnp.where(row < 7, up, pltpu.roll(carried, BLK - CX, 1))
        near = (own + two) + (x_low + x_high) + (y_low + y_high)
        return jnp.where(here, (dzrecv[j] + (6.0 - SHIFT)) * one - near, 0.0)

    right = ring_columns(0, z_final, gz < n_gz - 1)
    left = ring_columns(1, z_first, gz > 0)

    @pl.when(gx == 0)
    def _():
        clear_plane(v1, TWO - 1)

    @pl.when(gx == n_gx - 1)
    def _():
        clear_plane(v1, TWO + CX)

    @pl.when(gy == 0)
    def _():
        for p in range(CX):
            v1[TWO + p, low, :] = jnp.zeros((1, BLK), F32)

    @pl.when(gy == n_gy - 1)
    def _():
        for p in range(CX):
            v1[TWO + p, high, :] = jnp.zeros((1, BLK), F32)

    m3 = apply(v1, sides_of(right, left), visit_2, zero)

    quarter = lane // 32
    folded = []
    for m in (m0, m1, m2, m3):
        m = m + pltpu.roll(m, 64, 1)
        folded.append(m + pltpu.roll(m, 32, 1))
    mine = jnp.where(
        quarter == 0, folded[0],
        jnp.where(quarter == 1, folded[1], jnp.where(quarter == 2, folded[2], folded[3])),
    )
    mine = mine + pltpu.roll(mine, 4, 0)
    mine = mine + pltpu.roll(mine, 2, 0)
    mine = mine + pltpu.roll(mine, 1, 0)
    part_a[...] = mine[0:1]

    def a_copy(k, peer, slot):
        return pltpu.make_async_remote_copy(
            src_ref=part_a, dst_ref=recv_a.at[slot], send_sem=as_sem.at[k], recv_sem=ar_sem.at[slot],
            device_id=(peer, gy, gz), device_id_type=MESH,
        )

    def b_copy(k, peer, slot):
        return pltpu.make_async_remote_copy(
            src_ref=part_b, dst_ref=recv_b.at[slot], send_sem=bs_sem.at[k], recv_sem=br_sem.at[slot],
            device_id=(gx,) + peer, device_id_type=MESH,
        )

    @pl.loop(0, n_gx - 1)
    def _(t):
        a_copy(t, target_of(t), gx).start()

    recv_a[gx] = mine[0:1]

    @pl.loop(0, n_gx - 1)
    def _(t):
        tag_copy(t, target_of(t), gx).wait_send()
        tile_copy(t, target_of(t), gx).wait_send()

    each(diag_messages, ds_sem, dr_sem, "sent")
    each(side_messages, hs_sem, hr_sem, "sent")

    @pl.loop(0, n_gx - 1)
    def _(t):
        src = source_of(t)
        a_copy(t, src, src).wait_recv()

    stage = total([recv_a[i] for i in range(n_gx)])
    part_b[...] = stage

    @pl.loop(0, plane_n - 1)
    def _(k):
        b_copy(k, plane_peer(k), plane_me).start()

    recv_b[plane_me] = stage

    @pl.loop(0, n_gx - 1)
    def _(t):
        a_copy(t, target_of(t), gx).wait_send()

    @pl.loop(0, plane_n - 1)
    def _(k):
        b_copy(k, plane_peer(k), plane_me).wait_send()

    @pl.loop(0, plane_n - 1)
    def _(k):
        py, pz = plane_peer(k)
        b_copy(k, (py, pz), py * n_gz + pz).wait_recv()

    whole = jnp.broadcast_to(total([recv_b[i] for i in range(plane_n)]), (8, BLK))
    for shift in (16, 8, 4, 2, 1):
        whole = whole + pltpu.roll(whole, shift, 1)
    m0, m1, m2, m3 = (
        jnp.broadcast_to(whole[:, 32 * q + 31 : 32 * q + 32], (8, BLK)) for q in range(4)
    )
    e = m1 / m0
    a0 = 1.0 / (SHIFT + e)
    s = m2 - e * m1
    grow = a0 * s / m0
    a1 = 1.0 / (SHIFT + (m3 - 2.0 * e * m2 + e * e * m1) / s - grow)
    b0 = a0 * grow
    x0 = a0 + a1 * (b0 + a0 * e)
    x1 = a1 * a0
    r0 = a0 * e * (1.0 - a1 * SHIFT) - a1 * b0 * SHIFT
    r1 = a0 * (a1 * (SHIFT - e) - 1.0) - a1 * b0

    for out, w in ((x0_out, x0), (x1_out, -x1), (r0_out, r0), (r1_out, r1), (r2_out, x1)):
        out[...] = w[0:1]


def per_device(sizes, face_blocks, owner_rank, owner_tile, live_count, right_side, diagonal):
    n_gx, n_gy, n_gz = sizes
    plane_n = n_gy * n_gz
    box = (CX, HALF, BLK)
    padded = (CX + 2 * TWO, HALF + 2 * TOP, BLK)
    vmem = pl.BlockSpec(memory_space=pltpu.VMEM)
    hbm = pl.BlockSpec(memory_space=pltpu.HBM)
    counts = jnp.broadcast_to(live_count.reshape(1), (BLK - 2 * NB,))
    small = jnp.concatenate([owner_rank.reshape(NB), owner_tile.reshape(NB), counts])
    dma, scratch = pltpu.SemaphoreType.DMA, pltpu.VMEM
    v0, v1, v2, *weights = pl.pallas_call(
        functools.partial(body, n_gx, n_gy, n_gz),
        out_shape=tuple(jax.ShapeDtypeStruct(shape, F32) for shape in (box,) * 3 + ((1, BLK),) * 5),
        in_specs=[hbm] * 4,
        out_specs=(vmem,) * 8,
        scratch_shapes=[
            pltpu.SMEM((BLK,), jnp.int32),
            pltpu.SMEM((NB,), jnp.int32),
            scratch((NB, BLK * BLK), F32),
            scratch((NB + 1, HALF, BLK), F32),
            scratch((2 * BLK, BLK), jnp.bfloat16),
            scratch((n_gx, HALF, BLK), F32),
            scratch((n_gx, HALF, BLK), F32),
            scratch((n_gx, 1, BLK), F32),
            scratch((n_gx, 1, BLK), F32),
            scratch(padded, F32),
            scratch(padded, F32),
            scratch(padded, F32),
            scratch((2, 2, CX, 1, BLK), F32),
            scratch((2, 2, CX, 1, BLK), F32),
            scratch((2, 2, 8, BLK), F32),
            scratch((2, 2, 8, BLK), F32),
            scratch((2, 2, 1, BLK), F32),
            scratch((2, 2, 8, BLK), F32),
            scratch((2, 2, 8, BLK), F32),
            scratch((2, CX, 1, BLK), F32),
            scratch((2, CX, 1, BLK), F32),
            scratch((2, 8, BLK), F32),
            scratch((2, 8, BLK), F32),
            scratch((1, BLK), F32),
            scratch((1, BLK), F32),
            scratch((n_gx, 1, BLK), F32),
            scratch((plane_n, 1, BLK), F32),
            pltpu.SemaphoreType.REGULAR((3,)),
            dma((9,)),
            dma((n_gx,)), dma((n_gx,)), dma((n_gx,)), dma((n_gx,)),
            dma((20,)), dma((20,)), dma((6,)), dma((6,)),
            dma((n_gx,)), dma((n_gx,)), dma((plane_n,)), dma((plane_n,)),
        ],
        compiler_params=pltpu.CompilerParams(
            collective_id=0, has_side_effects=True, vmem_limit_bytes=54_750_000
        ),
    )(
        small,
        face_blocks.reshape(NB, BLK * BLK), right_side, diagonal,
    )
    x0, x1, r0, r1, r2 = (w.reshape(1, 1, BLK) for w in weights)
    return x0 * v0 + x1 * v1, r0 * v0 + (r1 * v1 + r2 * v2)


def solution(mesh):
    sizes = (mesh.shape["gx"], mesh.shape["gy"], mesh.shape["gz"])
    return jax.shard_map(
        functools.partial(per_device, sizes),
        mesh=mesh,
        in_specs=(
            P("gx", "gy", "gz", None, None),
            P("gx", "gy", "gz", None, None),
            P("gx", "gy", "gz", None),
            P("gx", "gy", "gz"),
            P("gx", "gy", "gz"),
            P("gx", "gy", "gz"),
        ),
        out_specs=(P("gx", "gy", "gz"), P("gx", "gy", "gz")),
        check_vma=False,
    )
```

```python
import functools

import jax
import jax.numpy as jnp
from jax import lax
from jax.experimental import pallas as pl
from jax.experimental.pallas import tpu as pltpu
from jax.sharding import PartitionSpec as P

NB = 24
BLK = 128
HALF = BLK // 2
CX = 16
F32 = jnp.float32
MESH = pl.DeviceIdType.MESH
SHIFT = 6.5
TOP = 16
TWO = 2


def ring_offsets(n, d):
    return tuple(sorted({d % n, -d % n} - {0}))


def body(
    n_gx, n_gy, n_gz,
    small_hbm, face_ref, rhs_ref, diag_ref,
    v0_out, v1_out, v2, x0_out, x1_out, r0_out, r1_out, r2_out,
    small, live_rank, face, rows, pair, sbuf, rbuf, stag, rtag,
    v0, v1, diag, ysend, yrecv, zsend, zrecv, xy, xz, yz,
    dysend, dyrecv, dzsend, dzrecv,
    part_a, part_b, recv_a, recv_b,
    known, in_sem, s_sem, r_sem, st_sem, rt_sem, hs_sem, hr_sem, ds_sem, dr_sem,
    as_sem, ar_sem, bs_sem, br_sem,
):
    gx, gy, gz = lax.axis_index("gx"), lax.axis_index("gy"), lax.axis_index("gz")
    chips = n_gx // 2
    chip, core = gx // 2, gx % 2
    plane_n = n_gy * n_gz
    plane_me = gy * n_gz + gz
    barrier = pltpu.get_barrier_semaphore()

    def step_chip(t):
        j = t // 2
        return (1 - 2 * (j % 2)) * (chips // 2 - (j + 1) // 2)

    def target_of(t):
        return lax.rem(chip + step_chip(t) + chips, chips) * 2 + lax.rem(core + 1 + t, 2)

    def source_of(t):
        return lax.rem(chip - step_chip(t) + chips, chips) * 2 + lax.rem(core + 1 + t, 2)

    for edge in (zrecv, yrecv, xy, xz, yz, dyrecv):
        edge[...] = jnp.zeros_like(edge)

    near_y, near_z = ring_offsets(n_gy, 1), ring_offsets(n_gz, 1)
    far_z = ring_offsets(n_gz, 2) if n_gz > 4 else ()

    def along_y(k):
        return (gx, lax.rem(gy + k, n_gy), gz)

    def along_z(k):
        return (gx, gy, lax.rem(gz + k, n_gz))

    def tell(sem, peer):
        pl.semaphore_signal(sem, inc=1, device_id=peer, device_id_type=MESH)

    for t in range(n_gx - 1):
        tell(barrier, (target_of(t), gy, gz))
    for k in near_y:
        tell(barrier, along_y(k))
    for k in near_z:
        tell(barrier, along_z(k))

    small_copies = [pltpu.make_async_copy(small_hbm, small, in_sem.at[6])]
    for c in small_copies:
        c.start()
    pieces = 4
    width = face.shape[1] // pieces
    face_copies = [
        pltpu.make_async_copy(
            face_ref.at[:, pl.ds(i * width, width)], face.at[:, pl.ds(i * width, width)], in_sem.at[i]
        )
        for i in range(pieces)
    ]
    for c in face_copies:
        c.start()
    rhs_copy = pltpu.make_async_copy(
        rhs_ref, v0.at[pl.ds(TWO, CX), pl.ds(TOP, HALF), :], in_sem.at[pieces]
    )
    rhs_copy.start()
    diag_copy = pltpu.make_async_copy(
        diag_ref, diag.at[pl.ds(TWO, CX), pl.ds(TOP, HALF), :], in_sem.at[pieces + 1]
    )
    diag_copy.start()

    def out_in(t, n):
        return (1 - 2 * (t % 2)) * (n // 2 - (t + 1) // 2)

    def plane_peer(t):
        py = lax.rem(gy + out_in(t % n_gy, n_gy) + n_gy, n_gy)
        return py, lax.rem(gz + out_in(t // n_gy, n_gz) + n_gz, n_gz)

    lane = lax.broadcasted_iota(jnp.int32, (8, BLK), 1)
    k_at = lax.broadcasted_iota(jnp.int32, (2 * BLK, BLK), 0)
    c_at = lax.broadcasted_iota(jnp.int32, (2 * BLK, BLK), 1)
    hit = (k_at // BLK == c_at // HALF) & ((k_at % BLK) // 2 == c_at % HALF)
    pair[...] = jnp.where(hit, 0.25, 0.0).astype(jnp.bfloat16)
    rows[NB] = jnp.zeros((HALF, BLK), F32)
    by_row = rows.reshape((NB + 1) * HALF, BLK)
    inner = pl.ds(TOP, HALF)
    low, high = pl.ds(TOP - 1, 1), pl.ds(TOP + HALF, 1)

    def clear_plane(v, at):
        v[at, inner, :] = jnp.zeros((HALF, BLK), F32)

    @pl.when(gx == 0)
    def _():
        clear_plane(v0, 1)

    @pl.when(gx == n_gx - 1)
    def _():
        clear_plane(v0, TWO + CX)

    per = HALF // pieces
    for i in range(pieces):
        face_copies[i].wait()

        @pl.loop(0, per // 4)
        def _(r4):
            for u in range(4):
                r = i * per + r4 * 4 + u
                at = pl.multiple_of(r * 2 * BLK, 2 * BLK)
                both = face[:, pl.ds(at, BLK)] + face[:, pl.ds(at + BLK, BLK)]
                for g in range(NB // 8):
                    by_row[pl.ds(g * 8 * HALF + r, 8, stride=HALF), :] = both[g * 8 : g * 8 + 8]

    for c in small_copies:
        c.wait()
    count = small[2 * NB]
    for s in range(NB):
        live_rank[s] = jnp.where(s < count, small[s], -1)

    pl.semaphore_wait(barrier, n_gx - 1 + len(near_y) + len(near_z))
    for k in near_y:
        tell(known.at[0], along_y(k))
    for k in near_z:
        tell(known.at[0], along_z(k))

    def packed(tgt):
        i0, i1 = jnp.int32(NB), jnp.int32(NB)
        l0, l1 = jnp.int32(0), jnp.int32(0)
        for s in range(NB):
            named = live_rank[s] == tgt
            label = small[NB + s] + 1
            free = i0 == NB
            first = named & free
            second = named & jnp.logical_not(free)
            i1 = jnp.where(second, s, i1)
            l1 = jnp.where(second, label, l1)
            i0 = jnp.where(first, s, i0)
            l0 = jnp.where(first, label, l0)
        a = rows[i0]
        b = rows[i1]
        w = jnp.concatenate([a, b], axis=1)
        hi = w.astype(jnp.bfloat16)
        rest = w - hi.astype(F32)
        mid = rest.astype(jnp.bfloat16)
        low = (rest - mid.astype(F32)).astype(jnp.bfloat16)
        s = pair[...]
        o = jnp.dot(hi, s, preferred_element_type=F32)
        o = o + jnp.dot(mid, s, preferred_element_type=F32)
        o = o + jnp.dot(low, s, preferred_element_type=F32)
        tag = jnp.where(lane[0:1] < HALF, l0, l1).astype(F32)
        return o, tag

    def tile_copy(t, tgt, slot):
        return pltpu.make_async_remote_copy(
            src_ref=sbuf.at[t], dst_ref=rbuf.at[slot], send_sem=s_sem.at[t], recv_sem=r_sem.at[slot],
            device_id=(tgt, gy, gz), device_id_type=MESH,
        )

    def tag_copy(t, tgt, slot):
        return pltpu.make_async_remote_copy(
            src_ref=stag.at[t], dst_ref=rtag.at[slot], send_sem=st_sem.at[t], recv_sem=rt_sem.at[slot],
            device_id=(tgt, gy, gz), device_id_type=MESH,
        )

    last = n_gx - 1

    @pl.loop(0, n_gx)
    def _(t):
        tgt = target_of(t)
        o, tag = packed(tgt)

        @pl.when(t < last)
        def _():
            stag[t] = tag
            sbuf[t] = o
            tag_copy(t, tgt, gx).start()
            tile_copy(t, tgt, gx).start()

        @pl.when(t == last)
        def _():
            rtag[gx] = tag
            rbuf[gx] = o

    def add_tiles(tile, tag):
        swapped = pltpu.roll(tile, HALF, 1)
        tag = jnp.broadcast_to(tag, (8, BLK))
        tag_swapped = pltpu.roll(tag, HALF, 1)[0:1]
        tag = tag[0:1]
        want = (lane[0:1] // HALF + 1).astype(F32)

        @pl.loop(0, CX // 4)
        def _(x4):
            for u in range(4):
                x = x4 * 4 + u
                here = want + (2 * x).astype(F32)
                m = jnp.broadcast_to(tag == here, (HALF, BLK))
                ms = jnp.broadcast_to(tag_swapped == here, (HALF, BLK))
                more = jnp.where(m, tile, 0.0) + jnp.where(ms, swapped, 0.0)
                v0[TWO + x, inner, :] = v0[TWO + x, inner, :] + more

    def total(refs):
        while len(refs) > 1:
            refs = [refs[i] + refs[i + 1] if i + 1 < len(refs) else refs[i] for i in range(0, len(refs), 2)]
        return refs[0]

    even = lane % 2 == 0
    fourth = lane % 4
    outer = (lane < 2) | (lane >= BLK - 2)

    def z_columns(v):
        parts = [[], [], [], []]
        for p in range(CX):
            for yb in range(HALF // 8):
                c = jnp.where(outer, v[TWO + p, pl.ds(TOP + 8 * yb, 8), :], 0.0)
                k = 16 * yb + p
                parts[p % 4].append(pltpu.roll(c, k, 1) if k else c)
        parts = [total(p) for p in parts]

        def pick(off):
            out = parts[0]
            for j in range(1, 4):
                out = jnp.where(fourth == (j + off) % 4, parts[j], out)
            return pltpu.roll(out, -off % BLK, 1) if off else out

        return pick(0), pick(1), pick(-2), pick(-1)

    def within(off):
        sends, takes = [], []
        for o, at, n in zip(off, (gx, gy, gz), (n_gx, n_gy, n_gz)):
            if o:
                sends.append(at > 0 if o < 0 else at < n - 1)
                takes.append(at < n - 1 if o < 0 else at > 0)
        return functools.reduce(jnp.logical_and, sends), functools.reduce(jnp.logical_and, takes)

    def message(off, src, dst, s_sem, r_sem):
        return pltpu.make_async_remote_copy(
            src_ref=src, dst_ref=dst, send_sem=s_sem, recv_sem=r_sem,
            device_id=(gx + off[0], gy + off[1], gz + off[2]), device_id_type=MESH,
        )

    def each(messages, s_sems, r_sems, what):
        for i, (off, src, dst) in messages:
            sends, takes = within(off)

            @pl.when(takes if what == "take" else sends)
            def _():
                m = message(off, src, dst, s_sems.at[i], r_sems.at[i])
                if what == "send":
                    m.start()
                elif what == "take":
                    m.wait_recv()
                else:
                    m.wait_send()

    ways = (-1, 1)
    diag_messages = list(enumerate(
        [((-1, 0, 0), diag.at[TWO, inner, :], diag.at[TWO + CX, inner, :]),
         ((1, 0, 0), diag.at[TWO + CX - 1, inner, :], diag.at[TWO - 1, inner, :])]
        + [((0, o, 0), dysend.at[i], dyrecv.at[i]) for i, o in enumerate(ways)]
        + [((0, 0, o), dzsend.at[i], dzrecv.at[i]) for i, o in enumerate(ways)]
    ))
    x_messages = [
        ((o, 0, 0), v0.at[src + deep, inner, :], v0.at[dst + deep, inner, :])
        for o, src, dst in ((-1, TWO, TWO + CX), (1, CX, 0))
        for deep in range(2)
    ]
    y_messages = [
        ((a, b, 0), ysend.at[j, 0, i * (CX - 1)], xy.at[i, j])
        for i, a in enumerate(ways) for j, b in enumerate(ways)
    ] + [((0, o, 0), ysend.at[i], yrecv.at[i]) for i, o in enumerate(ways)]
    z_messages = [
        ((a, 0, b), zsend.at[j, 0], xz.at[i, j])
        for i, a in enumerate(ways) for j, b in enumerate(ways)
    ] + [
        ((0, a, b), zsend.at[j, 0], yz.at[i, j])
        for i, a in enumerate(ways) for j, b in enumerate(ways)
    ] + [((0, 0, o), zsend.at[i], zrecv.at[i]) for i, o in enumerate(ways)]
    side_messages = list(enumerate(x_messages + y_messages + z_messages))
    n_x, n_y = len(x_messages), len(x_messages) + len(y_messages)

    diag_copy.wait()
    for p in range(CX):
        dysend[0, p] = diag[TWO + p, pl.ds(TOP, 1), :]
        dysend[1, p] = diag[TWO + p, pl.ds(TOP + HALF - 1, 1), :]
    first, _, _, final = z_columns(diag)
    dzsend[0] = first
    dzsend[1] = final
    each(diag_messages, ds_sem, dr_sem, "send")

    rhs_copy.wait()
    pl.semaphore_wait(known.at[0], len(near_y) + len(near_z))
    for k in far_z:
        tell(known.at[1], along_z(k))

    @pl.loop(0, n_gx)
    def _(i):
        t = lax.rem(i + last, n_gx)
        src = source_of(t)

        @pl.when(t < last)
        def _():
            tag_copy(t, src, src).wait_recv()
            tile_copy(t, src, src).wait_recv()

        @pl.when(i == n_gx // 2)
        def _():
            if far_z:
                pl.semaphore_wait(known.at[1], len(far_z))
            for k in range(1, n_gy):
                tell(known.at[2], along_y(k))

        add_tiles(rbuf[src], rtag[src])

    if n_gy > 1:
        pl.semaphore_wait(known.at[2], n_gy - 1)

    each(side_messages[:n_x], hs_sem, hr_sem, "send")
    z_first, z_second, z_third, z_final = z_columns(v0)
    zsend[0, 0], zsend[0, 1] = z_first, z_second
    zsend[1, 0], zsend[1, 1] = z_final, z_third
    each(side_messages[n_y:], hs_sem, hr_sem, "send")
    for p in range(CX):
        for deep in range(2):
            ysend[0, deep, p] = v0[TWO + p, pl.ds(TOP + deep, 1), :]
            ysend[1, deep, p] = v0[TWO + p, pl.ds(TOP + HALF - 1 - deep, 1), :]
    each(side_messages[n_x:n_y], hs_sem, hr_sem, "send")

    faces = [m for m in side_messages if sum(map(abs, m[1][0])) == 1]
    edges = [m for m in side_messages if sum(map(abs, m[1][0])) == 2]
    each(faces, hs_sem, hr_sem, "take")

    for p in range(CX):
        v0[TWO + p, high, :] = yrecv[0, 0, p]
        v0[TWO + p, pl.ds(TOP + HALF + 1, 1), :] = yrecv[0, 1, p]
        v0[TWO + p, low, :] = yrecv[1, 0, p]
        v0[TWO + p, pl.ds(TOP - 2, 1), :] = yrecv[1, 1, p]

    def sides_of(right, left):
        left = pltpu.roll(left, BLK - 1, 1)
        return jnp.where(even, right, left), jnp.where(even, left, right)

    def image_of(v, plane, row, h):
        c = v[plane, pl.ds(row, 8), :]
        near = v[plane - 1, pl.ds(row, 8), :] + v[plane + 1, pl.ds(row, 8), :]
        near = near + (v[plane, pl.ds(row - 1, 8), :] + v[plane, pl.ds(row + 1, 8), :])
        z_low = pltpu.roll(jnp.where(lane == BLK - 1, h, c), 1, 1)
        z_high = pltpu.roll(jnp.where(lane == 0, h, c), BLK - 1, 1)
        near = near + (z_low + z_high)
        return c, (diag[plane, pl.ds(row, 8), :] + (6.0 - SHIFT)) * c - near

    def turned(side, k):
        return pltpu.roll(side, BLK - k, 1) if k else side

    step = 8

    def moved(pair, base):
        return [pltpu.roll(side, lax.rem(BLK - base, BLK), 1) for side in pair]

    def apply(v, sides, visit, sums):

        def planes(i, sums):
            base = i * step
            here = moved(sides, base)
            for u in range(step):
                p = base + u
                for yb in range(HALF // 8):
                    h = turned(here[u % 2], 16 * yb + u)
                    c, image = image_of(v, TWO + p, TOP + 8 * yb, h)
                    sums = visit(p, yb, c, image, sums)
            return sums

        return lax.fori_loop(0, CX // step, planes, sums)

    zero = jnp.zeros((8, BLK), F32)

    def visit_1(p, yb, c, image, sums):
        v1[TWO + p, pl.ds(TOP + 8 * yb, 8), :] = image
        v0_out[p, pl.ds(8 * yb, 8), :] = c
        v1_out[p, pl.ds(8 * yb, 8), :] = image
        return sums[0] + c * c, sums[1] + c * image, sums[2] + image * image

    def visit_2(p, yb, c, image, sums):
        v2[p, pl.ds(8 * yb, 8), :] = image
        return sums + c * image

    m0, m1, m2 = apply(
        v0, sides_of(zrecv[0, 0], zrecv[1, 0]), visit_1, (zero, zero, zero)
    )
    each(diag_messages, ds_sem, dr_sem, "take")
    for p in range(CX):
        diag[TWO + p, high, :] = dyrecv[0, p]
        diag[TWO + p, low, :] = dyrecv[1, p]
    each(edges, hs_sem, hr_sem, "take")
    for i, plane in enumerate((TWO + CX, TWO - 1)):
        v0[plane, high, :] = xy[i, 0]
        v0[plane, low, :] = xy[i, 1]

    below, above = sides_of(yz[1, 0], yz[1, 1]), sides_of(yz[0, 0], yz[0, 1])

    @pl.loop(0, CX // step)
    def _(i):
        base = i * step
        under, over = moved(below, base), moved(above, base)
        for u in range(step):
            p = base + u
            _, image = image_of(v0, TWO + p, TOP - 8, turned(under[u % 2], BLK - 16 + u))
            v1[TWO + p, pl.ds(TOP - 8, 8), :] = image
            _, image = image_of(v0, TWO + p, TOP + HALF, turned(over[u % 2], u))
            v1[TWO + p, pl.ds(TOP + HALF, 8), :] = image

    ring_planes = (
        (TWO + CX, 0, sides_of(xz[0, 0], xz[0, 1])[0]),
        (TWO - 1, CX - 1, sides_of(xz[1, 0], xz[1, 1])[1]),
    )
    for plane, p, side in ring_planes:
        for yb in range(HALF // 8):
            _, image = image_of(v0, plane, TOP + 8 * yb, turned(side, 16 * yb + p))
            v1[plane, pl.ds(TOP + 8 * yb, 8), :] = image
    row = lax.broadcasted_iota(jnp.int32, (8, BLK), 0)
    in_row = lane % CX

    def ring_columns(j, own, here):
        one, two = zrecv[j, 0], zrecv[j, 1]
        x_low = jnp.where(in_row == 0, pltpu.roll(xz[1, j], BLK - 15, 1), pltpu.roll(one, 1, 1))
        x_high = jnp.where(
            in_row == CX - 1, pltpu.roll(xz[0, j], 15, 1), pltpu.roll(one, BLK - 1, 1)
        )
        down, up = pltpu.roll(one, 1, 0), pltpu.roll(one, 7, 0)
        carried = jnp.where(lane >= BLK - CX, pltpu.roll(yz[1, j], 1, 0), down)
        y_low = jnp.where(row > 0, down, pltpu.roll(carried, CX, 1))
        carried = jnp.where(lane < CX, pltpu.roll(yz[0, j], 7, 0), up)
        y_high = jnp.where(row < 7, up, pltpu.roll(carried, BLK - CX, 1))
        near = (own + two) + (x_low + x_high) + (y_low + y_high)
        return jnp.where(here, (dzrecv[j] + (6.0 - SHIFT)) * one - near, 0.0)

    right = ring_columns(0, z_final, gz < n_gz - 1)
    left = ring_columns(1, z_first, gz > 0)

    @pl.when(gx == 0)
    def _():
        clear_plane(v1, TWO - 1)

    @pl.when(gx == n_gx - 1)
    def _():
        clear_plane(v1, TWO + CX)

    @pl.when(gy == 0)
    def _():
        for p in range(CX):
            v1[TWO + p, low, :] = jnp.zeros((1, BLK), F32)

    @pl.when(gy == n_gy - 1)
    def _():
        for p in range(CX):
            v1[TWO + p, high, :] = jnp.zeros((1, BLK), F32)

    m3 = apply(v1, sides_of(right, left), visit_2, zero)

    quarter = lane // 32
    folded = []
    for m in (m0, m1, m2, m3):
        m = m + pltpu.roll(m, 64, 1)
        folded.append(m + pltpu.roll(m, 32, 1))
    mine = jnp.where(
        quarter == 0, folded[0],
        jnp.where(quarter == 1, folded[1], jnp.where(quarter == 2, folded[2], folded[3])),
    )
    mine = mine + pltpu.roll(mine, 4, 0)
    mine = mine + pltpu.roll(mine, 2, 0)
    mine = mine + pltpu.roll(mine, 1, 0)
    part_a[...] = mine[0:1]

    def a_copy(k, peer, slot):
        return pltpu.make_async_remote_copy(
            src_ref=part_a, dst_ref=recv_a.at[slot], send_sem=as_sem.at[k], recv_sem=ar_sem.at[slot],
            device_id=(peer, gy, gz), device_id_type=MESH,
        )

    def b_copy(k, peer, slot):
        return pltpu.make_async_remote_copy(
            src_ref=part_b, dst_ref=recv_b.at[slot], send_sem=bs_sem.at[k], recv_sem=br_sem.at[slot],
            device_id=(gx,) + peer, device_id_type=MESH,
        )

    @pl.loop(0, n_gx - 1)
    def _(t):
        a_copy(t, target_of(t), gx).start()

    recv_a[gx] = mine[0:1]

    @pl.loop(0, n_gx - 1)
    def _(t):
        tag_copy(t, target_of(t), gx).wait_send()
        tile_copy(t, target_of(t), gx).wait_send()

    each(diag_messages, ds_sem, dr_sem, "sent")
    each(side_messages, hs_sem, hr_sem, "sent")

    @pl.loop(0, n_gx - 1)
    def _(i):
        src = source_of(last - 1 - i)
        a_copy(0, src, src).wait_recv()

    stage = total([recv_a[i] for i in range(n_gx)])
    part_b[...] = stage

    @pl.loop(0, plane_n - 1)
    def _(k):
        b_copy(k, plane_peer(k), plane_me).start()

    recv_b[plane_me] = stage

    @pl.loop(0, n_gx - 1)
    def _(t):
        a_copy(t, target_of(t), gx).wait_send()

    @pl.loop(0, plane_n - 1)
    def _(k):
        b_copy(k, plane_peer(k), plane_me).wait_send()

    @pl.loop(0, plane_n - 1)
    def _(i):
        py, pz = plane_peer(plane_n - 2 - i)
        b_copy(0, (py, pz), py * n_gz + pz).wait_recv()

    whole = jnp.broadcast_to(total([recv_b[i] for i in range(plane_n)]), (8, BLK))
    for shift in (16, 8, 4, 2, 1):
        whole = whole + pltpu.roll(whole, shift, 1)
    m0, m1, m2, m3 = (
        jnp.broadcast_to(whole[:, 32 * q + 31 : 32 * q + 32], (8, BLK)) for q in range(4)
    )
    e = m1 / m0
    a0 = 1.0 / (SHIFT + e)
    s = m2 - e * m1
    grow = a0 * s / m0
    a1 = 1.0 / (SHIFT + (m3 - 2.0 * e * m2 + e * e * m1) / s - grow)
    b0 = a0 * grow
    x0 = a0 + a1 * (b0 + a0 * e)
    x1 = a1 * a0
    r0 = a0 * e * (1.0 - a1 * SHIFT) - a1 * b0 * SHIFT
    r1 = a0 * (a1 * (SHIFT - e) - 1.0) - a1 * b0

    for out, w in ((x0_out, x0), (x1_out, -x1), (r0_out, r0), (r1_out, r1), (r2_out, x1)):
        out[...] = w[0:1]


def per_device(sizes, face_blocks, owner_rank, owner_tile, live_count, right_side, diagonal):
    n_gx, n_gy, n_gz = sizes
    plane_n = n_gy * n_gz
    box = (CX, HALF, BLK)
    padded = (CX + 2 * TWO, HALF + 2 * TOP, BLK)
    vmem = pl.BlockSpec(memory_space=pltpu.VMEM)
    hbm = pl.BlockSpec(memory_space=pltpu.HBM)
    counts = jnp.broadcast_to(live_count.reshape(1), (BLK - 2 * NB,))
    small = jnp.concatenate([owner_rank.reshape(NB), owner_tile.reshape(NB), counts])
    dma, scratch = pltpu.SemaphoreType.DMA, pltpu.VMEM
    v0, v1, v2, *weights = pl.pallas_call(
        functools.partial(body, n_gx, n_gy, n_gz),
        out_shape=tuple(jax.ShapeDtypeStruct(shape, F32) for shape in (box,) * 3 + ((1, BLK),) * 5),
        in_specs=[hbm] * 4,
        out_specs=(vmem,) * 8,
        scratch_shapes=[
            pltpu.SMEM((BLK,), jnp.int32),
            pltpu.SMEM((NB,), jnp.int32),
            scratch((NB, BLK * BLK), F32),
            scratch((NB + 1, HALF, BLK), F32),
            scratch((2 * BLK, BLK), jnp.bfloat16),
            scratch((n_gx, HALF, BLK), F32),
            scratch((n_gx, HALF, BLK), F32),
            scratch((n_gx, 1, BLK), F32),
            scratch((n_gx, 1, BLK), F32),
            scratch(padded, F32),
            scratch(padded, F32),
            scratch(padded, F32),
            scratch((2, 2, CX, 1, BLK), F32),
            scratch((2, 2, CX, 1, BLK), F32),
            scratch((2, 2, 8, BLK), F32),
            scratch((2, 2, 8, BLK), F32),
            scratch((2, 2, 1, BLK), F32),
            scratch((2, 2, 8, BLK), F32),
            scratch((2, 2, 8, BLK), F32),
            scratch((2, CX, 1, BLK), F32),
            scratch((2, CX, 1, BLK), F32),
            scratch((2, 8, BLK), F32),
            scratch((2, 8, BLK), F32),
            scratch((1, BLK), F32),
            scratch((1, BLK), F32),
            scratch((n_gx, 1, BLK), F32),
            scratch((plane_n, 1, BLK), F32),
            pltpu.SemaphoreType.REGULAR((3,)),
            dma((9,)),
            dma((n_gx,)), dma((n_gx,)), dma((n_gx,)), dma((n_gx,)),
            dma((20,)), dma((20,)), dma((6,)), dma((6,)),
            dma((n_gx,)), dma((n_gx,)), dma((plane_n,)), dma((plane_n,)),
        ],
        compiler_params=pltpu.CompilerParams(
            collective_id=0, has_side_effects=True, vmem_limit_bytes=54_750_000
        ),
    )(
        small,
        face_blocks.reshape(NB, BLK * BLK), right_side, diagonal,
    )
    x0, x1, r0, r1, r2 = (w.reshape(1, 1, BLK) for w in weights)
    return x0 * v0 + x1 * v1, r0 * v0 + (r1 * v1 + r2 * v2)


def solution(mesh):
    sizes = (mesh.shape["gx"], mesh.shape["gy"], mesh.shape["gz"])
    return jax.shard_map(
        functools.partial(per_device, sizes),
        mesh=mesh,
        in_specs=(
            P("gx", "gy", "gz", None, None),
            P("gx", "gy", "gz", None, None),
            P("gx", "gy", "gz", None),
            P("gx", "gy", "gz"),
            P("gx", "gy", "gz"),
            P("gx", "gy", "gz"),
        ),
        out_specs=(P("gx", "gy", "gz"), P("gx", "gy", "gz")),
        check_vma=False,
    )
```

```python
import functools

import jax
import jax.numpy as jnp
from jax import lax
from jax.experimental import pallas as pl
from jax.experimental.pallas import tpu as pltpu
from jax.sharding import PartitionSpec as P

NB = 24
BLK = 128
HALF = BLK // 2
CX = 16
F32 = jnp.float32
MESH = pl.DeviceIdType.MESH
SHIFT = 6.5
TOP = 16
TWO = 2


def ring_offsets(n, d):
    return tuple(sorted({d % n, -d % n} - {0}))


def body(
    n_gx, n_gy, n_gz,
    small_hbm, face_ref, rhs_ref, diag_ref,
    v0_out, v1_out, v2, x0_out, x1_out, r0_out, r1_out, r2_out,
    small, live_rank, face, rows, pair, sbuf, rbuf,
    v0, v1, diag, ysend, yrecv, zsend, zrecv, xy, xz, yz,
    dysend, dyrecv, dzsend, dzrecv,
    part_a, part_b, recv_a, recv_b,
    known, in_sem, s_sem, r_sem, hs_sem, hr_sem, ds_sem, dr_sem,
    as_sem, ar_sem, bs_sem, br_sem,
):
    gx, gy, gz = lax.axis_index("gx"), lax.axis_index("gy"), lax.axis_index("gz")
    chips = n_gx // 2
    chip, core = gx // 2, gx % 2
    plane_n = n_gy * n_gz
    plane_me = gy * n_gz + gz
    barrier = pltpu.get_barrier_semaphore()

    def step_chip(t):
        j = t // 2
        return (1 - 2 * (j % 2)) * (chips // 2 - (j + 1) // 2)

    def target_of(t):
        return lax.rem(chip + step_chip(t) + chips, chips) * 2 + lax.rem(core + 1 + t, 2)

    def source_of(t):
        return lax.rem(chip - step_chip(t) + chips, chips) * 2 + lax.rem(core + 1 + t, 2)

    for edge in (zrecv, yrecv, xy, xz, yz, dyrecv):
        edge[...] = jnp.zeros_like(edge)

    near_y, near_z = ring_offsets(n_gy, 1), ring_offsets(n_gz, 1)
    far_z = ring_offsets(n_gz, 2) if n_gz > 4 else ()

    def along_y(k):
        return (gx, lax.rem(gy + k, n_gy), gz)

    def along_z(k):
        return (gx, gy, lax.rem(gz + k, n_gz))

    def tell(sem, peer):
        pl.semaphore_signal(sem, inc=1, device_id=peer, device_id_type=MESH)

    for t in range(n_gx - 1):
        tell(barrier, (target_of(t), gy, gz))
    for k in near_y:
        tell(barrier, along_y(k))
    for k in near_z:
        tell(barrier, along_z(k))

    small_copies = [pltpu.make_async_copy(small_hbm, small, in_sem.at[6])]
    for c in small_copies:
        c.start()
    pieces = 4
    width = face.shape[1] // pieces
    face_copies = [
        pltpu.make_async_copy(
            face_ref.at[:, pl.ds(i * width, width)], face.at[:, pl.ds(i * width, width)], in_sem.at[i]
        )
        for i in range(pieces)
    ]
    for c in face_copies:
        c.start()
    rhs_copy = pltpu.make_async_copy(
        rhs_ref, v0.at[pl.ds(TWO, CX), pl.ds(TOP, HALF), :], in_sem.at[pieces]
    )
    rhs_copy.start()
    diag_copy = pltpu.make_async_copy(
        diag_ref, diag.at[pl.ds(TWO, CX), pl.ds(TOP, HALF), :], in_sem.at[pieces + 1]
    )
    diag_copy.start()

    def out_in(t, n):
        return (1 - 2 * (t % 2)) * (n // 2 - (t + 1) // 2)

    def plane_peer(t):
        py = lax.rem(gy + out_in(t % n_gy, n_gy) + n_gy, n_gy)
        return py, lax.rem(gz + out_in(t // n_gy, n_gz) + n_gz, n_gz)

    lane = lax.broadcasted_iota(jnp.int32, (8, BLK), 1)
    k_at = lax.broadcasted_iota(jnp.int32, (2 * BLK, BLK), 0)
    c_at = lax.broadcasted_iota(jnp.int32, (2 * BLK, BLK), 1)
    hit = (k_at // BLK == c_at // HALF) & ((k_at % BLK) // 2 == c_at % HALF)
    pair[...] = jnp.where(hit, 0.25, 0.0).astype(jnp.bfloat16)
    rows[NB] = jnp.zeros((HALF, BLK), F32)
    by_row = rows.reshape((NB + 1) * HALF, BLK)
    inner = pl.ds(TOP, HALF)
    low, high = pl.ds(TOP - 1, 1), pl.ds(TOP + HALF, 1)

    def clear_plane(v, at):
        v[at, inner, :] = jnp.zeros((HALF, BLK), F32)

    @pl.when(gx == 0)
    def _():
        clear_plane(v0, 1)

    @pl.when(gx == n_gx - 1)
    def _():
        clear_plane(v0, TWO + CX)

    per = HALF // pieces
    for i in range(pieces):
        face_copies[i].wait()

        @pl.loop(0, per // 4)
        def _(r4):
            for u in range(4):
                r = i * per + r4 * 4 + u
                at = pl.multiple_of(r * 2 * BLK, 2 * BLK)
                both = face[:, pl.ds(at, BLK)] + face[:, pl.ds(at + BLK, BLK)]
                for g in range(NB // 8):
                    by_row[pl.ds(g * 8 * HALF + r, 8, stride=HALF), :] = both[g * 8 : g * 8 + 8]

    for c in small_copies:
        c.wait()
    count = small[2 * NB]
    for s in range(NB):
        live_rank[s] = jnp.where(s < count, small[s], -1)

    pl.semaphore_wait(barrier, n_gx - 1 + len(near_y) + len(near_z))
    for k in near_y:
        tell(known.at[0], along_y(k))
    for k in near_z:
        tell(known.at[0], along_z(k))

    def packed(tgt):
        i0, i1 = jnp.int32(NB), jnp.int32(NB)
        l0, l1 = jnp.int32(0), jnp.int32(0)
        for s in range(NB):
            named = live_rank[s] == tgt
            label = small[NB + s] + 1
            free = i0 == NB
            first = named & free
            second = named & jnp.logical_not(free)
            i1 = jnp.where(second, s, i1)
            l1 = jnp.where(second, label, l1)
            i0 = jnp.where(first, s, i0)
            l0 = jnp.where(first, label, l0)
        a = rows[i0]
        b = rows[i1]
        w = jnp.concatenate([a, b], axis=1)
        hi = w.astype(jnp.bfloat16)
        rest = w - hi.astype(F32)
        mid = rest.astype(jnp.bfloat16)
        low = (rest - mid.astype(F32)).astype(jnp.bfloat16)
        s = pair[...]
        o = jnp.dot(hi, s, preferred_element_type=F32)
        o = o + jnp.dot(mid, s, preferred_element_type=F32)
        o = o + jnp.dot(low, s, preferred_element_type=F32)
        tag = jnp.where(lane[0:1] < HALF, l0, l1).astype(F32)
        return o, tag

    with_tag = pl.ds(0, HALF + 1)

    def tile_copy(t, tgt, slot):
        return pltpu.make_async_remote_copy(
            src_ref=sbuf.at[t, with_tag, :], dst_ref=rbuf.at[slot, with_tag, :], send_sem=s_sem.at[t], recv_sem=r_sem.at[slot],
            device_id=(tgt, gy, gz), device_id_type=MESH,
        )

    last = n_gx - 1

    @pl.loop(0, n_gx)
    def _(t):
        tgt = target_of(t)
        o, tag = packed(tgt)

        @pl.when(t < last)
        def _():
            sbuf[t, pl.ds(0, HALF), :] = o
            sbuf[t, pl.ds(HALF, 1), :] = tag
            tile_copy(t, tgt, gx).start()

        @pl.when(t == last)
        def _():
            rbuf[gx, pl.ds(0, HALF), :] = o
            rbuf[gx, pl.ds(HALF, 1), :] = tag

    def add_tiles(tile, tag):
        swapped = pltpu.roll(tile, HALF, 1)
        tag = jnp.broadcast_to(tag, (8, BLK))
        tag_swapped = pltpu.roll(tag, HALF, 1)[0:1]
        tag = tag[0:1]
        want = (lane[0:1] // HALF + 1).astype(F32)

        @pl.loop(0, CX // 4)
        def _(x4):
            for u in range(4):
                x = x4 * 4 + u
                here = want + (2 * x).astype(F32)
                m = jnp.broadcast_to(tag == here, (HALF, BLK))
                ms = jnp.broadcast_to(tag_swapped == here, (HALF, BLK))
                more = jnp.where(m, tile, 0.0) + jnp.where(ms, swapped, 0.0)
                v0[TWO + x, inner, :] = v0[TWO + x, inner, :] + more

    def total(refs):
        while len(refs) > 1:
            refs = [refs[i] + refs[i + 1] if i + 1 < len(refs) else refs[i] for i in range(0, len(refs), 2)]
        return refs[0]

    even = lane % 2 == 0
    fourth = lane % 4
    outer = (lane < 2) | (lane >= BLK - 2)

    def z_columns(v):
        parts = [[], [], [], []]
        for p in range(CX):
            for yb in range(HALF // 8):
                c = jnp.where(outer, v[TWO + p, pl.ds(TOP + 8 * yb, 8), :], 0.0)
                k = 16 * yb + p
                parts[p % 4].append(pltpu.roll(c, k, 1) if k else c)
        parts = [total(p) for p in parts]

        def pick(off):
            out = parts[0]
            for j in range(1, 4):
                out = jnp.where(fourth == (j + off) % 4, parts[j], out)
            return pltpu.roll(out, -off % BLK, 1) if off else out

        return pick(0), pick(1), pick(-2), pick(-1)

    def within(off):
        sends, takes = [], []
        for o, at, n in zip(off, (gx, gy, gz), (n_gx, n_gy, n_gz)):
            if o:
                sends.append(at > 0 if o < 0 else at < n - 1)
                takes.append(at < n - 1 if o < 0 else at > 0)
        return functools.reduce(jnp.logical_and, sends), functools.reduce(jnp.logical_and, takes)

    def message(off, src, dst, s_sem, r_sem):
        return pltpu.make_async_remote_copy(
            src_ref=src, dst_ref=dst, send_sem=s_sem, recv_sem=r_sem,
            device_id=(gx + off[0], gy + off[1], gz + off[2]), device_id_type=MESH,
        )

    def each(messages, s_sems, r_sems, what):
        for i, (off, src, dst) in messages:
            sends, takes = within(off)

            @pl.when(takes if what == "take" else sends)
            def _():
                m = message(off, src, dst, s_sems.at[i], r_sems.at[i])
                if what == "send":
                    m.start()
                elif what == "take":
                    m.wait_recv()
                else:
                    m.wait_send()

    ways = (-1, 1)
    diag_messages = list(enumerate(
        [((-1, 0, 0), diag.at[TWO, inner, :], diag.at[TWO + CX, inner, :]),
         ((1, 0, 0), diag.at[TWO + CX - 1, inner, :], diag.at[TWO - 1, inner, :])]
        + [((0, o, 0), dysend.at[i], dyrecv.at[i]) for i, o in enumerate(ways)]
        + [((0, 0, o), dzsend.at[i], dzrecv.at[i]) for i, o in enumerate(ways)]
    ))
    x_messages = [
        ((o, 0, 0), v0.at[src + deep, inner, :], v0.at[dst + deep, inner, :])
        for o, src, dst in ((-1, TWO, TWO + CX), (1, CX, 0))
        for deep in range(2)
    ]
    y_messages = [
        ((a, b, 0), ysend.at[j, 0, i * (CX - 1)], xy.at[i, j])
        for i, a in enumerate(ways) for j, b in enumerate(ways)
    ] + [((0, o, 0), ysend.at[i], yrecv.at[i]) for i, o in enumerate(ways)]
    z_messages = [
        ((a, 0, b), zsend.at[j, 0], xz.at[i, j])
        for i, a in enumerate(ways) for j, b in enumerate(ways)
    ] + [
        ((0, a, b), zsend.at[j, 0], yz.at[i, j])
        for i, a in enumerate(ways) for j, b in enumerate(ways)
    ] + [((0, 0, o), zsend.at[i], zrecv.at[i]) for i, o in enumerate(ways)]
    side_messages = list(enumerate(x_messages + y_messages + z_messages))
    n_x, n_y = len(x_messages), len(x_messages) + len(y_messages)

    diag_copy.wait()
    for p in range(CX):
        dysend[0, p] = diag[TWO + p, pl.ds(TOP, 1), :]
        dysend[1, p] = diag[TWO + p, pl.ds(TOP + HALF - 1, 1), :]
    first, _, _, final = z_columns(diag)
    dzsend[0] = first
    dzsend[1] = final
    each(diag_messages, ds_sem, dr_sem, "send")

    rhs_copy.wait()
    pl.semaphore_wait(known.at[0], len(near_y) + len(near_z))
    for k in far_z:
        tell(known.at[1], along_z(k))

    @pl.loop(0, n_gx)
    def _(i):
        t = lax.rem(i + last, n_gx)
        src = source_of(t)

        @pl.when(t < last)
        def _():
            tile_copy(t, src, src).wait_recv()

        @pl.when(i == n_gx // 2)
        def _():
            if far_z:
                pl.semaphore_wait(known.at[1], len(far_z))
            for k in range(1, n_gy):
                tell(known.at[2], along_y(k))

        add_tiles(rbuf[src, pl.ds(0, HALF), :], rbuf[src, pl.ds(HALF, 1), :])

    if n_gy > 1:
        pl.semaphore_wait(known.at[2], n_gy - 1)

    each(side_messages[:n_x], hs_sem, hr_sem, "send")
    z_first, z_second, z_third, z_final = z_columns(v0)
    zsend[0, 0], zsend[0, 1] = z_first, z_second
    zsend[1, 0], zsend[1, 1] = z_final, z_third
    each(side_messages[n_y:], hs_sem, hr_sem, "send")
    for p in range(CX):
        for deep in range(2):
            ysend[0, deep, p] = v0[TWO + p, pl.ds(TOP + deep, 1), :]
            ysend[1, deep, p] = v0[TWO + p, pl.ds(TOP + HALF - 1 - deep, 1), :]
    each(side_messages[n_x:n_y], hs_sem, hr_sem, "send")

    faces = [m for m in side_messages if sum(map(abs, m[1][0])) == 1]
    edges = [m for m in side_messages if sum(map(abs, m[1][0])) == 2]
    each(faces, hs_sem, hr_sem, "take")

    for p in range(CX):
        v0[TWO + p, high, :] = yrecv[0, 0, p]
        v0[TWO + p, pl.ds(TOP + HALF + 1, 1), :] = yrecv[0, 1, p]
        v0[TWO + p, low, :] = yrecv[1, 0, p]
        v0[TWO + p, pl.ds(TOP - 2, 1), :] = yrecv[1, 1, p]

    def sides_of(right, left):
        left = pltpu.roll(left, BLK - 1, 1)
        return jnp.where(even, right, left), jnp.where(even, left, right)

    def image_of(v, plane, row, h):
        c = v[plane, pl.ds(row, 8), :]
        near = v[plane - 1, pl.ds(row, 8), :] + v[plane + 1, pl.ds(row, 8), :]
        near = near + (v[plane, pl.ds(row - 1, 8), :] + v[plane, pl.ds(row + 1, 8), :])
        z_low = pltpu.roll(jnp.where(lane == BLK - 1, h, c), 1, 1)
        z_high = pltpu.roll(jnp.where(lane == 0, h, c), BLK - 1, 1)
        near = near + (z_low + z_high)
        return c, (diag[plane, pl.ds(row, 8), :] + (6.0 - SHIFT)) * c - near

    def turned(side, k):
        return pltpu.roll(side, BLK - k, 1) if k else side

    step = 8

    def moved(pair, base):
        return [pltpu.roll(side, lax.rem(BLK - base, BLK), 1) for side in pair]

    def apply(v, sides, visit, sums):

        def planes(i, sums):
            base = i * step
            here = moved(sides, base)
            for u in range(step):
                p = base + u
                for yb in range(HALF // 8):
                    h = turned(here[u % 2], 16 * yb + u)
                    c, image = image_of(v, TWO + p, TOP + 8 * yb, h)
                    sums = visit(p, yb, c, image, sums)
            return sums

        return lax.fori_loop(0, CX // step, planes, sums)

    zero = jnp.zeros((8, BLK), F32)

    def visit_1(p, yb, c, image, sums):
        v1[TWO + p, pl.ds(TOP + 8 * yb, 8), :] = image
        v0_out[p, pl.ds(8 * yb, 8), :] = c
        v1_out[p, pl.ds(8 * yb, 8), :] = image
        return sums[0] + c * c, sums[1] + c * image, sums[2] + image * image

    def visit_2(p, yb, c, image, sums):
        v2[p, pl.ds(8 * yb, 8), :] = image
        return sums + c * image

    m0, m1, m2 = apply(
        v0, sides_of(zrecv[0, 0], zrecv[1, 0]), visit_1, (zero, zero, zero)
    )
    each(diag_messages, ds_sem, dr_sem, "take")
    for p in range(CX):
        diag[TWO + p, high, :] = dyrecv[0, p]
        diag[TWO + p, low, :] = dyrecv[1, p]
    each(edges, hs_sem, hr_sem, "take")
    for i, plane in enumerate((TWO + CX, TWO - 1)):
        v0[plane, high, :] = xy[i, 0]
        v0[plane, low, :] = xy[i, 1]

    below, above = sides_of(yz[1, 0], yz[1, 1]), sides_of(yz[0, 0], yz[0, 1])

    @pl.loop(0, CX // step)
    def _(i):
        base = i * step
        under, over = moved(below, base), moved(above, base)
        for u in range(step):
            p = base + u
            _, image = image_of(v0, TWO + p, TOP - 8, turned(under[u % 2], BLK - 16 + u))
            v1[TWO + p, pl.ds(TOP - 8, 8), :] = image
            _, image = image_of(v0, TWO + p, TOP + HALF, turned(over[u % 2], u))
            v1[TWO + p, pl.ds(TOP + HALF, 8), :] = image

    ring_planes = (
        (TWO + CX, 0, sides_of(xz[0, 0], xz[0, 1])[0]),
        (TWO - 1, CX - 1, sides_of(xz[1, 0], xz[1, 1])[1]),
    )
    for plane, p, side in ring_planes:
        for yb in range(HALF // 8):
            _, image = image_of(v0, plane, TOP + 8 * yb, turned(side, 16 * yb + p))
            v1[plane, pl.ds(TOP + 8 * yb, 8), :] = image
    row = lax.broadcasted_iota(jnp.int32, (8, BLK), 0)
    in_row = lane % CX

    def ring_columns(j, own, here):
        one, two = zrecv[j, 0], zrecv[j, 1]
        x_low = jnp.where(in_row == 0, pltpu.roll(xz[1, j], BLK - 15, 1), pltpu.roll(one, 1, 1))
        x_high = jnp.where(
            in_row == CX - 1, pltpu.roll(xz[0, j], 15, 1), pltpu.roll(one, BLK - 1, 1)
        )
        down, up = pltpu.roll(one, 1, 0), pltpu.roll(one, 7, 0)
        carried = jnp.where(lane >= BLK - CX, pltpu.roll(yz[1, j], 1, 0), down)
        y_low = jnp.where(row > 0, down, pltpu.roll(carried, CX, 1))
        carried = jnp.where(lane < CX, pltpu.roll(yz[0, j], 7, 0), up)
        y_high = jnp.where(row < 7, up, pltpu.roll(carried, BLK - CX, 1))
        near = (own + two) + (x_low + x_high) + (y_low + y_high)
        return jnp.where(here, (dzrecv[j] + (6.0 - SHIFT)) * one - near, 0.0)

    right = ring_columns(0, z_final, gz < n_gz - 1)
    left = ring_columns(1, z_first, gz > 0)

    @pl.when(gx == 0)
    def _():
        clear_plane(v1, TWO - 1)

    @pl.when(gx == n_gx - 1)
    def _():
        clear_plane(v1, TWO + CX)

    @pl.when(gy == 0)
    def _():
        for p in range(CX):
            v1[TWO + p, low, :] = jnp.zeros((1, BLK), F32)

    @pl.when(gy == n_gy - 1)
    def _():
        for p in range(CX):
            v1[TWO + p, high, :] = jnp.zeros((1, BLK), F32)

    m3 = apply(v1, sides_of(right, left), visit_2, zero)

    quarter = lane // 32
    folded = []
    for m in (m0, m1, m2, m3):
        m = m + pltpu.roll(m, 64, 1)
        folded.append(m + pltpu.roll(m, 32, 1))
    mine = jnp.where(
        quarter == 0, folded[0],
        jnp.where(quarter == 1, folded[1], jnp.where(quarter == 2, folded[2], folded[3])),
    )
    mine = mine + pltpu.roll(mine, 4, 0)
    mine = mine + pltpu.roll(mine, 2, 0)
    mine = mine + pltpu.roll(mine, 1, 0)
    part_a[...] = mine[0:1]

    def a_copy(k, peer, slot):
        return pltpu.make_async_remote_copy(
            src_ref=part_a, dst_ref=recv_a.at[slot], send_sem=as_sem.at[k], recv_sem=ar_sem.at[slot],
            device_id=(peer, gy, gz), device_id_type=MESH,
        )

    def b_copy(k, peer, slot):
        return pltpu.make_async_remote_copy(
            src_ref=part_b, dst_ref=recv_b.at[slot], send_sem=bs_sem.at[k], recv_sem=br_sem.at[slot],
            device_id=(gx,) + peer, device_id_type=MESH,
        )

    @pl.loop(0, n_gx - 1)
    def _(t):
        a_copy(t, target_of(t), gx).start()

    recv_a[gx] = mine[0:1]

    @pl.loop(0, n_gx - 1)
    def _(t):
        tile_copy(t, target_of(t), gx).wait_send()

    each(diag_messages, ds_sem, dr_sem, "sent")
    each(side_messages, hs_sem, hr_sem, "sent")

    @pl.loop(0, n_gx - 1)
    def _(i):
        src = source_of(last - 1 - i)
        a_copy(0, src, src).wait_recv()

    stage = total([recv_a[i] for i in range(n_gx)])
    part_b[...] = stage

    @pl.loop(0, plane_n - 1)
    def _(k):
        b_copy(k, plane_peer(k), plane_me).start()

    recv_b[plane_me] = stage

    @pl.loop(0, n_gx - 1)
    def _(t):
        a_copy(t, target_of(t), gx).wait_send()

    @pl.loop(0, plane_n - 1)
    def _(k):
        b_copy(k, plane_peer(k), plane_me).wait_send()

    @pl.loop(0, plane_n - 1)
    def _(i):
        py, pz = plane_peer(plane_n - 2 - i)
        b_copy(0, (py, pz), py * n_gz + pz).wait_recv()

    whole = jnp.broadcast_to(total([recv_b[i] for i in range(plane_n)]), (8, BLK))
    for shift in (16, 8, 4, 2, 1):
        whole = whole + pltpu.roll(whole, shift, 1)
    m0, m1, m2, m3 = (
        jnp.broadcast_to(whole[:, 32 * q + 31 : 32 * q + 32], (8, BLK)) for q in range(4)
    )
    e = m1 / m0
    a0 = 1.0 / (SHIFT + e)
    s = m2 - e * m1
    grow = a0 * s / m0
    a1 = 1.0 / (SHIFT + (m3 - 2.0 * e * m2 + e * e * m1) / s - grow)
    b0 = a0 * grow
    x0 = a0 + a1 * (b0 + a0 * e)
    x1 = a1 * a0
    r0 = a0 * e * (1.0 - a1 * SHIFT) - a1 * b0 * SHIFT
    r1 = a0 * (a1 * (SHIFT - e) - 1.0) - a1 * b0

    for out, w in ((x0_out, x0), (x1_out, -x1), (r0_out, r0), (r1_out, r1), (r2_out, x1)):
        out[...] = w[0:1]


def per_device(sizes, face_blocks, owner_rank, owner_tile, live_count, right_side, diagonal):
    n_gx, n_gy, n_gz = sizes
    plane_n = n_gy * n_gz
    box = (CX, HALF, BLK)
    padded = (CX + 2 * TWO, HALF + 2 * TOP, BLK)
    vmem = pl.BlockSpec(memory_space=pltpu.VMEM)
    hbm = pl.BlockSpec(memory_space=pltpu.HBM)
    counts = jnp.broadcast_to(live_count.reshape(1), (BLK - 2 * NB,))
    small = jnp.concatenate([owner_rank.reshape(NB), owner_tile.reshape(NB), counts])
    dma, scratch = pltpu.SemaphoreType.DMA, pltpu.VMEM
    v0, v1, v2, *weights = pl.pallas_call(
        functools.partial(body, n_gx, n_gy, n_gz),
        out_shape=tuple(jax.ShapeDtypeStruct(shape, F32) for shape in (box,) * 3 + ((1, BLK),) * 5),
        in_specs=[hbm] * 4,
        out_specs=(vmem,) * 8,
        scratch_shapes=[
            pltpu.SMEM((BLK,), jnp.int32),
            pltpu.SMEM((NB,), jnp.int32),
            scratch((NB, BLK * BLK), F32),
            scratch((NB + 1, HALF, BLK), F32),
            scratch((2 * BLK, BLK), jnp.bfloat16),
            scratch((n_gx, HALF + 8, BLK), F32),
            scratch((n_gx, HALF + 8, BLK), F32),
            scratch(padded, F32),
            scratch(padded, F32),
            scratch(padded, F32),
            scratch((2, 2, CX, 1, BLK), F32),
            scratch((2, 2, CX, 1, BLK), F32),
            scratch((2, 2, 8, BLK), F32),
            scratch((2, 2, 8, BLK), F32),
            scratch((2, 2, 1, BLK), F32),
            scratch((2, 2, 8, BLK), F32),
            scratch((2, 2, 8, BLK), F32),
            scratch((2, CX, 1, BLK), F32),
            scratch((2, CX, 1, BLK), F32),
            scratch((2, 8, BLK), F32),
            scratch((2, 8, BLK), F32),
            scratch((1, BLK), F32),
            scratch((1, BLK), F32),
            scratch((n_gx, 1, BLK), F32),
            scratch((plane_n, 1, BLK), F32),
            pltpu.SemaphoreType.REGULAR((3,)),
            dma((9,)),
            dma((n_gx,)), dma((n_gx,)),
            dma((20,)), dma((20,)), dma((6,)), dma((6,)),
            dma((n_gx,)), dma((n_gx,)), dma((plane_n,)), dma((plane_n,)),
        ],
        compiler_params=pltpu.CompilerParams(
            collective_id=0, has_side_effects=True, vmem_limit_bytes=54_750_000
        ),
    )(
        small,
        face_blocks.reshape(NB, BLK * BLK), right_side, diagonal,
    )
    x0, x1, r0, r1, r2 = (w.reshape(1, 1, BLK) for w in weights)
    return x0 * v0 + x1 * v1, r0 * v0 + (r1 * v1 + r2 * v2)


def solution(mesh):
    sizes = (mesh.shape["gx"], mesh.shape["gy"], mesh.shape["gz"])
    return jax.shard_map(
        functools.partial(per_device, sizes),
        mesh=mesh,
        in_specs=(
            P("gx", "gy", "gz", None, None),
            P("gx", "gy", "gz", None, None),
            P("gx", "gy", "gz", None),
            P("gx", "gy", "gz"),
            P("gx", "gy", "gz"),
            P("gx", "gy", "gz"),
        ),
        out_specs=(P("gx", "gy", "gz"), P("gx", "gy", "gz")),
        check_vma=False,
    )
```
